256 devices in a mesh: island: 4 (over z_lo), fsdp: 64 (over z_hi, x, y, core).
Axes of the slice: x: 4, y: 4, z: 8 (z_hi: 2, z_lo: 4; z = z_hi * 4 + z_lo), core: 2. Of those that a mesh axis runs over, the one named last changes fastest.
Arguments:
- grads: bfloat16 [4, 1, 14336, 4096], P('island', None, 'fsdp'), may hold values from -200 to 200
- buffer: bfloat16 [4, 14336, 4096], P('island', 'fsdp'), may hold values from -200 to 200
- q_old: float32 [4, 4096, 128], P('island', 'fsdp'), may hold values from -0.09375 to 0.09375
- anchor: bfloat16 [14336, 4096], P('fsdp'), may hold values from -6 to 6
- momentum: float32 [14336, 4096], P(('fsdp', 'island')), may hold values from -6 to 6
Outputs:
- anchor_new: bfloat16 [14336, 4096], P('fsdp')
- buffer_new: bfloat16 [4, 14336, 4096], P('island', 'fsdp')
- momentum_new: float32 [14336, 4096], P(('fsdp', 'island'))
The draws below stay inside these ranges and needn't reach their ends.
All inputs are finite; a program needn't handle non-finite values.
Results may differ from the reference program's by a relative error of at most 0.012.
Values may be sent and summed in bfloat16 or wider, within the bound.
A program may use at most 64 MiB of HBM per device.

```python
import math
import jax
import jax.numpy as jnp
from jax import lax

ROWS = 14336
COLS = 4096
RANK = 128
STEPS = 1
ISLANDS = 4
N_ISLAND = 4


def scale_tables(key):
    base_key = jax.random.fold_in(key, 7)
    row_key, col_key = jax.random.split(base_key)
    rising_rows = 10.0 ** (jnp.arange(ROWS, dtype=jnp.float32) / ROWS)
    rising_cols = 10.0 ** (jnp.arange(COLS, dtype=jnp.float32) / COLS)
    row_scale = rising_rows * jax.random.uniform(row_key, (ROWS,), jnp.float32, 1.0, 2.0) / 5.0
    col_scale = rising_cols * jax.random.uniform(col_key, (COLS,), jnp.float32, 1.0, 2.0) / 5.0
    return (row_scale, col_scale)


def scaled_noise(key, salt, layers):
    noise_key = jax.random.fold_in(key, salt)
    row_scale, col_scale = scale_tables(key)
    shape = (ISLANDS, layers, ROWS, COLS)
    values = jnp.clip(jax.random.normal(noise_key, shape, jnp.float32), -4.0, 4.0)
    return values * row_scale[:, None] * col_scale[None, :]


def draw_grads(key, part):
    return scaled_noise(key, 21, STEPS).astype(jnp.bfloat16)


def draw_buffer(key, part):
    return scaled_noise(key, 22, 1).reshape(ISLANDS, ROWS, COLS).astype(jnp.bfloat16)


def levels(key, dims, shards, low, high):
    factor_of, own = 1.0, jax.random.fold_in(key, 6)
    for axis_at, shards_of in shards:
        draws = jnp.exp(jax.random.uniform(jax.random.fold_in(own, axis_at), (shards_of,), jnp.float32, low / len(shards), high / len(shards)))
        factor_of = factor_of * jnp.repeat(draws, dims[axis_at] // shards_of).reshape([-1 if axis == axis_at else 1 for axis in range(len(dims))])
    return factor_of


def centred(rng, extent, spread, most, cuts=(), held_as=jnp.bfloat16):
    values = spread * jax.random.normal(rng, extent, jnp.float32)
    if cuts:
        values = values * levels(rng, extent, cuts, -0.22, 0.18)
    return jnp.clip(values, -most, most).astype(held_as)


def setup_inputs(seed: int = 0) -> dict:
    keys = jax.random.split(jax.random.key(seed), 6)
    grads = draw_grads(jax.random.fold_in(keys[5], 71), 0)
    buffer = draw_buffer(jax.random.fold_in(keys[5], 71), 0)
    q_old = centred(keys[2], (ISLANDS, COLS, RANK), COLS ** -0.5, 0.09375, ((0, 4), (1, 64)), jnp.float32)
    anchor = centred(keys[3], (ROWS, COLS), 1.0, 6.0, ((0, 64),))
    momentum = centred(keys[4], (ROWS, COLS), 1.0, 6.0, ((0, 256),), jnp.float32)
    return {"grads": grads, "buffer": buffer, "q_old": q_old, "anchor": anchor, "momentum": momentum}


precise = lax.Precision.HIGHEST
error_decay = 0.95
outer_beta = 0.9
outer_rate = 0.7
epsilon = 1e-06

def product(left_side, right_side, left_dims, right_dims):
    return lax.dot_general(left_side.astype(jnp.float32), right_side.astype(jnp.float32), (((left_dims,), (right_dims,)), ((), ())), precision=precise, preferred_element_type=jnp.float32)

def inverse_upper(lower_factor):
    identity = jnp.eye(lower_factor.shape[0], dtype=lower_factor.dtype)
    return lax.linalg.triangular_solve(lower_factor, identity, left_side=True, lower=True, transpose_a=True)

def island_window(island_args):
    grad_steps, buffer_one, q_basis = island_args
    residue = buffer_one.astype(jnp.float32)
    moved_sum = jnp.zeros(residue.shape, jnp.float32)
    rate = math.sqrt(ROWS * COLS / RANK)
    for step_index in range(STEPS):
        matrix = residue + grad_steps[step_index].astype(jnp.float32)
        raw_image = product(matrix, q_basis, 1, 0)
        gram_matrix = product(raw_image, raw_image, 0, 0)
        upper_inverse = inverse_upper(jnp.linalg.cholesky(gram_matrix))
        basis_rows = product(raw_image, upper_inverse, 1, 0)
        factor = product(matrix, basis_rows, 0, 0)
        q_basis = factor / jnp.sqrt(lax.optimization_barrier(jnp.sum(factor * factor, axis=0)) + epsilon)
        residue = matrix - (1.0 - error_decay) * product(basis_rows, factor, 1, 1)
        moved_sum = moved_sum + rate * product(basis_rows, q_basis, 1, 1)
    return (moved_sum.astype(jnp.bfloat16), residue.astype(jnp.bfloat16))

def reference(grads, buffer, q_old, anchor, momentum):
    deltas, residues = lax.map(island_window, (grads, buffer, q_old))
    delta_total = lax.optimization_barrier(jnp.sum(deltas, axis=0, dtype=jnp.float32))
    delta_mean = delta_total / N_ISLAND
    momentum_new = outer_beta * momentum + delta_mean
    anchor_new = (anchor.astype(jnp.float32) - outer_rate * (delta_mean + outer_beta * momentum_new)).astype(jnp.bfloat16)
    return (anchor_new, residues, momentum_new)
```

```python
import math

import jax
import jax.numpy as jnp
from jax import lax
from jax.experimental import pallas as pl
from jax.experimental.pallas import tpu as pltpu
from jax.sharding import Mesh
from jax.sharding import PartitionSpec as P

ROWS = 14336
COLS = 4096
RANK = 128
FSDP = ("fsdp_0", "fsdp_1", "fsdp_2", "fsdp_3")
FSDP_ISLAND = ("fsdp_0", "fsdp_1", "fsdp_2", "fsdp_3", "island")
OWN = 224
PADDED = 256
QUARTER = 56
QUARTER_PADDED = 64
STEP_COLS = 512
MESH = pl.DeviceIdType.MESH

precise = lax.Precision.HIGHEST
error_decay = 0.95
outer_beta = 0.9
outer_rate = 0.7
epsilon = 1e-06
f32 = jnp.float32
bf16 = jnp.bfloat16


def dot(left, right, left_dim, right_dim, precision=None):
    return lax.dot_general(
        left,
        right,
        (((left_dim,), (right_dim,)), ((), ())),
        precision=precision,
        preferred_element_type=f32,
    )


def inverse_lower(gram, width=2):
    n = gram.shape[0]
    rest = gram
    side = (
        lax.broadcasted_iota(jnp.int32, (n, n), 0) == lax.broadcasted_iota(jnp.int32, (n, n), 1)
    ).astype(f32)
    done = []
    for first in range(0, n, 8):
        rows = lax.broadcasted_iota(jnp.int32, rest.shape, 0)
        scale = jnp.ones((8, n), f32)
        head = lax.broadcasted_iota(jnp.int32, (8, n), 0)
        for at in range(0, 8, width):
            columns = [
                jnp.broadcast_to(rest[:, first + at + i : first + at + i + 1], rest.shape)
                for i in range(width)
            ]
            for i in range(width):
                row = at + i
                pivot = columns[i][row : row + 1, :]
                times = jnp.where(rows > row, columns[i] * (1.0 / pivot), 0.0)
                scale = jnp.where(head == row, pivot, scale)
                for j in range(i + 1, width):
                    columns[j] = columns[j] - times * columns[j][row : row + 1, :]
                rest = rest - times * rest[row : row + 1, :]
                side = side - times * side[row : row + 1, :]
        done.append(side[:8] * lax.rsqrt(scale))
        rest, side = rest[8:], side[8:]
    return jnp.concatenate(done, axis=0)


def exchange_kernel(
    grads,
    buffer,
    q_old,
    momentum,
    f_all,
    p_scaled,
    p_own,
    mom_all,
    grads_v,
    buffer_v,
    mom_v,
    mb,
    qa,
    raw_b,
    gsend,
    g1,
    g2,
    g3,
    g4,
    gfull,
    rp,
    rown,
    r1,
    s1,
    r2,
    s2,
    s2b,
    r3,
    s3b,
    r4,
    p_all,
    squares,
    load_sem,
    send_sem,
    recv_sem,
):
    c = lax.axis_index("island")
    h = lax.axis_index("fsdp_0")
    x = lax.axis_index("fsdp_1")
    y = lax.axis_index("fsdp_2")
    k = lax.axis_index("fsdp_3")
    z = h * 4 + c
    a = x * (1 - k) + y * k
    b = y * (1 - k) + x * k

    def first_axis(d):
        return {"fsdp_1": lax.rem(x + d * (1 - k), 4), "fsdp_2": lax.rem(y + d * k, 4)}

    def second_axis(d):
        return {"fsdp_1": lax.rem(x + d * k, 4), "fsdp_2": lax.rem(y + d * (1 - k), 4)}

    def along_z(d):
        to = lax.rem(z + d, 8)
        return {"fsdp_0": to // 4, "island": lax.rem(to, 4)}

    other_core = {"fsdp_3": 1 - k}
    other_half = {"fsdp_0": 1 - h}

    peers = [other_core, other_half]
    for d in (1, 2, 3):
        peers.append({"fsdp_1": lax.rem(x + d, 4)})
        peers.append({"fsdp_2": lax.rem(y + d, 4)})
        peers.append({"fsdp_0": 1 - h, "fsdp_1": lax.rem(x + d, 4)})
        peers.append({"island": lax.rem(c + d, 4)})
    for d in (1, 2, 6, 7):
        peers.append(along_z(d))

    counter = [0]
    started = []

    def copy_to(src, dst, device):
        at = counter[0]
        counter[0] += 1
        copy = pltpu.make_async_remote_copy(
            src_ref=src,
            dst_ref=dst,
            send_sem=send_sem.at[at],
            recv_sem=recv_sem.at[at],
            device_id=device,
            device_id_type=MESH,
        )
        return copy

    def send(src, dst, device):
        copy = copy_to(src, dst, device)
        copy.start()
        started.append(copy)
        return copy

    barrier = pltpu.get_barrier_semaphore()
    for peer in peers:
        pl.semaphore_signal(barrier, inc=1, device_id=peer, device_id_type=MESH)

    loads = [
        pltpu.make_async_copy(momentum, mom_v, load_sem.at[0]),
        pltpu.make_async_copy(grads, grads_v, load_sem.at[1]),
        pltpu.make_async_copy(buffer, buffer_v, load_sem.at[2]),
    ]
    for load in loads:
        load.start()
    qa[h, x, y, k] = q_old[...].astype(bf16)
    loads[0].wait()
    mom_all[c] = jnp.concatenate(
        [mom_v[...], jnp.zeros((QUARTER_PADDED - QUARTER, COLS), f32)], axis=0
    ).astype(bf16)
    pl.semaphore_wait(barrier, len(peers))

    own_piece = qa.at[h, x, y, k]
    q_copies = {}
    for dh in (0, 1):
        for dx in (1, 2, 3) if dh == 0 else (0, 1, 2, 3):
            q_copies[dh, dx] = send(
                own_piece,
                own_piece,
                {"fsdp_0": lax.rem(h + dh, 2), "fsdp_1": lax.rem(x + dx, 4)},
            )

    line = []
    for step in (1, 2, 3):
        up_ok = jnp.logical_and(c < 3, c >= step - 1)
        down_ok = jnp.logical_and(c > 0, c + step - 1 <= 3)
        up_at = lax.rem(c - (step - 1) + 4, 4)
        down_at = lax.rem(c + (step - 1), 4)
        up = copy_to(mom_all.at[up_at], mom_all.at[up_at], {"island": lax.rem(c + 1, 4)})
        down = copy_to(mom_all.at[down_at], mom_all.at[down_at], {"island": lax.rem(c + 3, 4)})
        line.append((up_ok, up, c - step >= 0, down_ok, down, c + step <= 3))

    def line_send(step):
        up_ok, up, _, down_ok, down, _ = line[step - 1]

        @pl.when(up_ok)
        def _():
            up.start()

        @pl.when(down_ok)
        def _():
            down.start()

    def line_receive(step):
        up_ok, up, from_below, down_ok, down, from_above = line[step - 1]

        @pl.when(from_below)
        def _():
            up.wait_recv()

        @pl.when(from_above)
        def _():
            down.wait_recv()

        @pl.when(up_ok)
        def _():
            up.wait_send()

        @pl.when(down_ok)
        def _():
            down.wait_send()

    line_send(1)

    loads[1].wait()
    loads[2].wait()

    @pl.loop(0, OWN // 16)
    def _(i):
        at = pl.ds(pl.multiple_of(i * 16, 16), 16)
        mb[at, :] = (grads_v[at, :].astype(f32) + buffer_v[at, :].astype(f32)).astype(bf16)

    mb[OWN:, :] = jnp.zeros((PADDED - OWN, COLS), bf16)

    up_y = {"fsdp_2": lax.rem(y + 1, 4)}
    down_y = {"fsdp_2": lax.rem(y + 3, 4)}
    below, above = lax.rem(y + 3, 4), lax.rem(y + 1, 4)
    q_ring = []
    for group in (0, 1):
        at = lax.rem(h + group, 2)
        for dx in (1, 2, 3) if group == 0 else (0, 1, 2, 3):
            q_copies[group, dx].wait_recv()
        mine = qa.at[at, :, y, k]
        q_ring.append((at, send(mine, mine, up_y), send(mine, mine, down_y)))
    q_forward = []
    for at, up, down in q_ring:
        up.wait_recv()
        came = qa.at[at, 0:2, below, k]
        on_up = send(came, came, up_y)
        down.wait_recv()
        came = qa.at[at, 2:4, above, k]
        on_down = send(came, came, down_y)
        q_forward.append((at, on_up, on_down))
    q_cross = []
    for at, on_up, on_down in q_forward:
        on_up.wait_recv()
        on_down.wait_recv()
        half = qa.at[at, :, :, k]
        q_cross.append((at, send(half, half, other_core)))

    raw = jnp.zeros((PADDED, RANK), f32)
    for at, copy in q_cross:
        copy.wait_recv()
        columns = pl.ds(pl.multiple_of(at * (COLS // 2), COLS // 2), COLS // 2)
        raw = raw + dot(mb[:, columns], qa[at].reshape(COLS // 2, RANK), 1, 0)
    raw_b[...] = raw.astype(bf16)
    raw_rows = raw_b[...]

    gram = dot(raw_rows, raw_rows, 0, 0)
    gsend[0] = gram[:64]
    gsend[1] = gram[64:]
    gram_cross = send(gsend.at[1 - k], g1, other_core)

    raw_t = raw.T.astype(bf16)

    def image(half, part, store):
        columns = pl.ds(pl.multiple_of(half * (COLS // 2) + part * 256, 256), 256)
        block = dot(raw_t, mb[:, columns], 1, 0)
        store(part * 2, block[:, :128])
        store(part * 2 + 1, block[:, 128:])

    def store_far(at, block):
        rp[at] = block.astype(bf16)

    def store_near(at, block):
        rown[at] = block

    r_cross = []
    for chunk in (0, 1):
        for part in range(chunk * 4, chunk * 4 + 4):
            image(1 - k, part, store_far)
        piece = pl.ds(chunk * 8, 8)
        r_cross.append(send(rp.at[piece], r1.at[piece], other_core))

    gram_cross.wait_recv()
    g2[a] = gsend[k] + g1[...]
    gram_first = [send(g2.at[a], g2.at[a], first_axis(d)) for d in (2, 1, 3)]

    for part in range(8):
        image(k, part, store_near)

    for copy in r_cross:
        copy.wait_recv()
    r_first = []
    for d in (2, 1, 3):
        to = lax.rem(a + d, 4)
        for j in range(4):
            s1[d - 1, j] = (rown[to * 4 + j] + r1[to * 4 + j].astype(f32)).astype(bf16)
        r_first.append(send(s1.at[d - 1], r2.at[d - 1], first_axis(d)))

    line_receive(1)
    line_send(2)

    for copy in gram_first:
        copy.wait_recv()
    g3[b] = (g2[0] + g2[1]) + (g2[2] + g2[3])
    gram_second = [send(g3.at[b], g3.at[b], second_axis(d)) for d in (2, 1, 3)]

    for copy in r_first:
        copy.wait_recv()
    for j in range(4):
        s2[j] = (rown[a * 4 + j] + r1[a * 4 + j].astype(f32)) + (
            (r2[0, j].astype(f32) + r2[1, j].astype(f32)) + r2[2, j].astype(f32)
        )
    r_second = []
    for d in (2, 1, 3):
        s2b[d - 1] = s2[lax.rem(b + d, 4)].astype(bf16)
        r_second.append(send(s2b.at[d - 1], r3.at[d - 1], second_axis(d)))

    for copy in gram_second:
        copy.wait_recv()
    g4[h] = (g3[0] + g3[1]) + (g3[2] + g3[3])
    gram_third = send(g4.at[h], g4.at[h], other_half)

    for copy in r_second:
        copy.wait_recv()
    s3b[...] = (
        s2[b] + ((r3[0].astype(f32) + r3[1].astype(f32)) + r3[2].astype(f32))
    ).astype(bf16)
    r_third = send(s3b, r4, other_half)

    gram_third.wait_recv()
    gfull[k] = g4[0] + g4[1]
    gram_last = send(gfull.at[k], gfull.at[k], other_core)
    line_receive(2)
    line_send(3)
    gram_last.wait_recv()
    lower = inverse_lower(jnp.concatenate([gfull[0], gfull[1]], axis=0))

    r_third.wait_recv()
    image_sum = s3b[...].astype(f32) + r4[...].astype(f32)
    f_all[k, a, b, c] = dot(lower, image_sum, 1, 0, precise).astype(bf16)

    mine = f_all.at[k, a, b, c]
    z_copies = [send(mine, mine, along_z(d)) for d in (2, 1, 7)]
    basis = dot(raw_rows.astype(f32), lower, 1, 1, precise)[:OWN]
    p_all[c] = basis.astype(bf16)
    p_copies = [send(p_all.at[c], p_all.at[c], {"island": lax.rem(c + d, 4)}) for d in (1, 2, 3)]
    p_own[...] = (basis * (error_decay - 1.0)).astype(bf16)

    up_a, down_a = first_axis(1), first_axis(3)
    up_b, down_b = second_axis(1), second_axis(3)
    a_below, a_above = lax.rem(a + 3, 4), lax.rem(a + 1, 4)
    b_below, b_above, b_far = lax.rem(b + 3, 4), lax.rem(b + 1, 4), lax.rem(b + 2, 4)

    def ring_a(at):
        piece = f_all.at[k, a, at]
        return (at, send(piece, piece, up_a), send(piece, piece, down_a))

    def forward_a(ring):
        at, up, down = ring
        up.wait_recv()
        came = f_all.at[k, a_below, at, 0:2]
        on_up = send(came, came, up_a)
        down.wait_recv()
        came = f_all.at[k, a_above, at, 2:4]
        on_down = send(came, came, down_a)
        return (at, on_up, on_down)

    def cross(ring):
        at, on_up, on_down = ring
        on_up.wait_recv()
        on_down.wait_recv()
        part = f_all.at[k, :, at]
        return send(part, part, other_core)

    for copy in z_copies:
        copy.wait_recv()
    piece = f_all.at[k, a, b]
    up, down = send(piece, piece, up_b), send(piece, piece, down_b)
    ring_own = ring_a(b)
    up.wait_recv()
    came = f_all.at[k, a, b_below, 0:2]
    on_up = send(came, came, up_b)
    down.wait_recv()
    came = f_all.at[k, a, b_above, 2:4]
    on_down = send(came, came, down_b)
    ring_below = ring_a(b_below)
    ring_above = ring_a(b_above)
    own_on = forward_a(ring_own)
    on_up.wait_recv()
    on_down.wait_recv()
    ring_far = ring_a(b_far)
    below_on = forward_a(ring_below)
    above_on = forward_a(ring_above)
    crossing = [cross(own_on)]
    far_on = forward_a(ring_far)
    crossing.append(cross(below_on))
    crossing.append(cross(above_on))
    line_receive(3)
    crossing.append(cross(far_on))
    for copy in crossing:
        copy.wait_recv()

    squares[...] = jnp.zeros_like(squares)

    @pl.loop(0, 8)
    def _(i):
        for j in range(4):
            for island in range(4):
                values = f_all[i // 4, lax.rem(i, 4), j, island].astype(f32)
                squares[island] += values * values

    ones = jnp.ones((8, RANK), f32)
    for copy in p_copies:
        copy.wait_recv()
    rate = math.sqrt(ROWS * COLS / RANK) / 4.0
    for island in range(4):
        total = dot(ones, squares[island], 1, 1, precise)[:1]
        scale = rate * lax.rsqrt(total + epsilon)
        p_scaled[:, island * RANK : (island + 1) * RANK] = (
            p_all[island].astype(f32) * scale
        ).astype(bf16)
    for copy in started:
        copy.wait_send()


def exchange(grads, buffer, q_old, momentum):
    vmem = pltpu.VMEM
    whole = pl.BlockSpec(memory_space=pltpu.VMEM)
    anywhere = pl.BlockSpec(memory_space=pl.ANY)
    block = (128, 128)
    return pl.pallas_call(
        exchange_kernel,
        out_shape=(
            jax.ShapeDtypeStruct((2, 4, 4, 4, 128, 128), bf16),
            jax.ShapeDtypeStruct((OWN, 4 * RANK), bf16),
            jax.ShapeDtypeStruct((OWN, RANK), bf16),
            jax.ShapeDtypeStruct((4, QUARTER_PADDED, COLS), bf16),
        ),
        in_specs=[anywhere, anywhere, whole, anywhere],
        out_specs=(whole, whole, whole, whole),
        scratch_shapes=[
            vmem((OWN, COLS), bf16),
            vmem((OWN, COLS), bf16),
            vmem((QUARTER, COLS), f32),
            vmem((PADDED, COLS), bf16),
            vmem((2, 4, 4, 2, 64, RANK), bf16),
            vmem((PADDED, RANK), bf16),
            vmem((2, 64, 128), f32),
            vmem((64, 128), f32),
            vmem((4, 64, 128), f32),
            vmem((4, 64, 128), f32),
            vmem((2, 64, 128), f32),
            vmem((2, 64, 128), f32),
            vmem((16, *block), bf16),
            vmem((16, *block), f32),
            vmem((16, *block), bf16),
            vmem((3, 4, *block), bf16),
            vmem((3, 4, *block), bf16),
            vmem((4, *block), f32),
            vmem((3, *block), bf16),
            vmem((3, *block), bf16),
            vmem(block, bf16),
            vmem(block, bf16),
            vmem((4, OWN, RANK), bf16),
            vmem((4, *block), f32),
            pltpu.SemaphoreType.DMA((3,)),
            pltpu.SemaphoreType.DMA((80,)),
            pltpu.SemaphoreType.DMA((80,)),
        ],
        compiler_params=pltpu.CompilerParams(collective_id=0, has_side_effects=True),
        name="exchange",
    )(grads, buffer, q_old, momentum)


def update_kernel(
    factors, p_scaled, p_own, mom_all, grads, buffer, anchor, momentum, anchor_new, buffer_new, momentum_new, means
):
    c = lax.axis_index("island")
    pieces = STEP_COLS // 128
    for pair in range(0, pieces, 2):
        at = slice(pair * 128, pair * 128 + 256)
        both = jnp.concatenate(
            [factors[pair + i].reshape(4 * RANK, 128) for i in (0, 1)], axis=1
        )
        means[:, at] = dot(p_scaled[...], both, 1, 0)
        own = jnp.concatenate([factors[pair + i, c] for i in (0, 1)], axis=1)
        matrix = grads[:, at].astype(f32) + buffer[:, at].astype(f32)
        buffer_new[:, at] = (matrix + dot(p_own[...], own, 1, 0)).astype(bf16)
    carried = jnp.concatenate(
        [mom_all[i].astype(f32)[:QUARTER] for i in range(4)], axis=0
    )
    mean = means[...]
    anchor_new[...] = (
        anchor[...].astype(f32)
        - outer_rate * (mean + outer_beta * (outer_beta * carried + mean))
    ).astype(bf16)
    rows = pl.ds(pl.multiple_of(c * QUARTER, 8), QUARTER)
    momentum_new[...] = outer_beta * momentum[...] + means[rows, :]


def update(factors, p_scaled, p_own, mom_all, grads, buffer, anchor, momentum):
    wide = pl.BlockSpec((OWN, STEP_COLS), lambda i: (0, i))
    narrow = pl.BlockSpec((QUARTER, STEP_COLS), lambda i: (0, i))
    return pl.pallas_call(
        update_kernel,
        grid=(COLS // STEP_COLS,),
        out_shape=(
            jax.ShapeDtypeStruct((OWN, COLS), bf16),
            jax.ShapeDtypeStruct((OWN, COLS), bf16),
            jax.ShapeDtypeStruct((QUARTER, COLS), f32),
        ),
        in_specs=[
            pl.BlockSpec((STEP_COLS // 128, 4, 128, 128), lambda i: (i, 0, 0, 0)),
            pl.BlockSpec((OWN, 4 * RANK), lambda i: (0, 0)),
            pl.BlockSpec((OWN, RANK), lambda i: (0, 0)),
            pl.BlockSpec((4, QUARTER_PADDED, STEP_COLS), lambda i: (0, 0, i)),
            wide,
            wide,
            wide,
            narrow,
        ],
        out_specs=(wide, wide, narrow),
        scratch_shapes=[pltpu.VMEM((OWN, STEP_COLS), f32)],
        name="update",
    )(factors, p_scaled, p_own, mom_all, grads, buffer, anchor, momentum)


def body(grads, buffer, q_old, anchor, momentum):
    grads, buffer = grads[0, 0], buffer[0]
    f_all, p_scaled, p_own, mom_all = exchange(grads, buffer, q_old[0], momentum)
    factors = f_all.reshape(COLS // 128, 4, 128, 128)
    anchor_new, buffer_new, momentum_new = update(
        factors, p_scaled, p_own, mom_all, grads, buffer, anchor, momentum
    )
    return (anchor_new, buffer_new[None], momentum_new)


def solution(mesh):
    split = Mesh(
        mesh.devices.reshape(mesh.shape["island"], 2, 4, 4, 2),
        ("island", "fsdp_0", "fsdp_1", "fsdp_2", "fsdp_3"),
    )
    return jax.shard_map(
        body,
        mesh=split,
        in_specs=(
            P("island", None, FSDP, None),
            P("island", FSDP, None),
            P("island", FSDP, None),
            P(FSDP, None),
            P(FSDP_ISLAND, None),
        ),
        out_specs=(P(FSDP, None), P("island", FSDP, None), P(FSDP_ISLAND, None)),
        check_vma=False,
    )
```

```python
import math

import jax
import jax.numpy as jnp
from jax import lax
from jax.experimental import pallas as pl
from jax.experimental.pallas import tpu as pltpu
from jax.sharding import Mesh
from jax.sharding import PartitionSpec as P

ROWS = 14336
COLS = 4096
RANK = 128
FSDP = ("fsdp_0", "fsdp_1", "fsdp_2", "fsdp_3")
FSDP_ISLAND = ("fsdp_0", "fsdp_1", "fsdp_2", "fsdp_3", "island")
OWN = 224
PADDED = 256
QUARTER = 56
MESH = pl.DeviceIdType.MESH

precise = lax.Precision.HIGHEST
error_decay = 0.95
outer_beta = 0.9
outer_rate = 0.7
epsilon = 1e-06
f32 = jnp.float32
bf16 = jnp.bfloat16


def dot(left, right, left_dim, right_dim, precision=None):
    return lax.dot_general(
        left,
        right,
        (((left_dim,), (right_dim,)), ((), ())),
        precision=precision,
        preferred_element_type=f32,
    )


def inverse_lower(gram, width=8):
    n = gram.shape[0]
    rest = gram
    side = (
        lax.broadcasted_iota(jnp.int32, (n, n), 0) == lax.broadcasted_iota(jnp.int32, (n, n), 1)
    ).astype(f32)
    done = []
    for first in range(0, n, 8):
        rows = lax.broadcasted_iota(jnp.int32, rest.shape, 0)
        scale = jnp.ones((8, n), f32)
        head = lax.broadcasted_iota(jnp.int32, (8, n), 0)
        for at in range(0, 8, width):
            columns = [
                jnp.broadcast_to(rest[:, first + at + i : first + at + i + 1], rest.shape)
                for i in range(width)
            ]
            for i in range(width):
                row = at + i
                pivot = columns[i][row : row + 1, :]
                times = jnp.where(rows > row, columns[i] * (1.0 / pivot), 0.0)
                scale = jnp.where(head == row, pivot, scale)
                for j in range(i + 1, width):
                    columns[j] = columns[j] - times * columns[j][row : row + 1, :]
                rest = rest - times * rest[row : row + 1, :]
                side = side - times * side[row : row + 1, :]
        done.append(side[:8] * lax.rsqrt(scale))
        rest, side = rest[8:], side[8:]
    return jnp.concatenate(done, axis=0)


def exchange_kernel(
    grads,
    buffer,
    q_old,
    anchor,
    momentum,
    anchor_new,
    buffer_new,
    momentum_new,
    f_all,
    p_scaled,
    p_own,
    mom_all,
    anchor_v,
    means,
    nb,
    na,
    nk,
    q_v,
    grads_v,
    buffer_v,
    mom_v,
    mb,
    qa,
    raw_b,
    gsend,
    g1,
    g2,
    g3,
    g4,
    gfull,
    rp,
    rown,
    r1,
    s1,
    r2,
    s2,
    s2b,
    r3,
    s3b,
    r4,
    p_all,
    load_sem,
    send_sem,
    recv_sem,
):
    c = lax.axis_index("island")
    h = lax.axis_index("fsdp_0")
    x = lax.axis_index("fsdp_1")
    y = lax.axis_index("fsdp_2")
    k = lax.axis_index("fsdp_3")
    z = h * 4 + c
    a = x * (1 - k) + y * k
    b = y * (1 - k) + x * k

    def first_axis(d):
        return {"fsdp_1": lax.rem(x + d * (1 - k), 4), "fsdp_2": lax.rem(y + d * k, 4)}

    def second_axis(d):
        return {"fsdp_1": lax.rem(x + d * k, 4), "fsdp_2": lax.rem(y + d * (1 - k), 4)}

    def along_z(d):
        to = lax.rem(z + d, 8)
        return {"fsdp_0": to // 4, "island": lax.rem(to, 4)}

    other_core = {"fsdp_3": 1 - k}
    other_half = {"fsdp_0": 1 - h}

    peers = [other_core, other_half]
    for d in (1, 2, 3):
        peers.append({"fsdp_1": lax.rem(x + d, 4)})
        peers.append({"fsdp_2": lax.rem(y + d, 4)})
        peers.append({"fsdp_0": 1 - h, "fsdp_1": lax.rem(x + d, 4)})
        peers.append({"island": lax.rem(c + d, 4)})
    for d in (1, 2, 6, 7):
        peers.append(along_z(d))

    counter = [0]
    started = []

    def copy_to(src, dst, device):
        at = counter[0]
        counter[0] += 1
        copy = pltpu.make_async_remote_copy(
            src_ref=src,
            dst_ref=dst,
            send_sem=send_sem.at[at],
            recv_sem=recv_sem.at[at],
            device_id=device,
            device_id_type=MESH,
        )
        return copy

    def send(src, dst, device):
        copy = copy_to(src, dst, device)
        copy.start()
        started.append(copy)
        return copy

    barrier = pltpu.get_barrier_semaphore()
    for peer in peers:
        pl.semaphore_signal(barrier, inc=1, device_id=peer, device_id_type=MESH)

    loads = [
        pltpu.make_async_copy(momentum, mom_v, load_sem.at[0]),
        pltpu.make_async_copy(grads, grads_v, load_sem.at[1]),
        pltpu.make_async_copy(buffer, buffer_v, load_sem.at[2]),
        pltpu.make_async_copy(anchor, anchor_v, load_sem.at[3]),
        pltpu.make_async_copy(q_old, q_v, load_sem.at[4]),
    ]
    for at in (4, 0, 1, 2, 3):
        loads[at].start()
    loads[4].wait()
    qa[h, x, y, k] = q_v[...].astype(bf16)
    loads[0].wait()
    mom_all[c] = mom_v[...].astype(bf16)
    pl.semaphore_wait(barrier, len(peers))

    own_piece = qa.at[h, x, y, k]
    q_copies = {}
    for dh in (0, 1):
        for dx in (1, 2, 3) if dh == 0 else (0, 1, 2, 3):
            q_copies[dh, dx] = send(
                own_piece,
                own_piece,
                {"fsdp_0": lax.rem(h + dh, 2), "fsdp_1": lax.rem(x + dx, 4)},
            )

    line = []
    for step in (1, 2, 3):
        up_ok = jnp.logical_and(c < 3, c >= step - 1)
        down_ok = jnp.logical_and(c > 0, c + step - 1 <= 3)
        up_at = lax.rem(c - (step - 1) + 4, 4)
        down_at = lax.rem(c + (step - 1), 4)
        up = copy_to(mom_all.at[up_at], mom_all.at[up_at], {"island": lax.rem(c + 1, 4)})
        down = copy_to(mom_all.at[down_at], mom_all.at[down_at], {"island": lax.rem(c + 3, 4)})
        line.append((up_ok, up, c - step >= 0, down_ok, down, c + step <= 3))

    def line_send(step):
        up_ok, up, _, down_ok, down, _ = line[step - 1]

        @pl.when(up_ok)
        def _():
            up.start()

        @pl.when(down_ok)
        def _():
            down.start()

    def line_receive(step):
        up_ok, up, from_below, down_ok, down, from_above = line[step - 1]

        @pl.when(from_below)
        def _():
            up.wait_recv()

        @pl.when(from_above)
        def _():
            down.wait_recv()

        @pl.when(up_ok)
        def _():
            up.wait_send()

        @pl.when(down_ok)
        def _():
            down.wait_send()

    line_send(1)

    loads[1].wait()
    loads[2].wait()

    @pl.loop(0, OWN // 16)
    def _(i):
        at = pl.ds(pl.multiple_of(i * 16, 16), 16)
        mb[at, :] = (grads_v[at, :].astype(f32) + buffer_v[at, :].astype(f32)).astype(bf16)

    mb[OWN:, :] = jnp.zeros((PADDED - OWN, COLS), bf16)

    up_y = {"fsdp_2": lax.rem(y + 1, 4)}
    down_y = {"fsdp_2": lax.rem(y + 3, 4)}
    below, above = lax.rem(y + 3, 4), lax.rem(y + 1, 4)
    q_ring = []
    for group in (0, 1):
        at = lax.rem(h + group, 2)
        for dx in (1, 2, 3) if group == 0 else (0, 1, 2, 3):
            q_copies[group, dx].wait_recv()
        mine = qa.at[at, :, y, k]
        q_ring.append((at, send(mine, mine, up_y), send(mine, mine, down_y)))
    q_forward = []
    for at, up, down in q_ring:
        up.wait_recv()
        came = qa.at[at, 0:2, below, k]
        on_up = send(came, came, up_y)
        down.wait_recv()
        came = qa.at[at, 2:4, above, k]
        on_down = send(came, came, down_y)
        q_forward.append((at, on_up, on_down))
    q_cross = []
    for at, on_up, on_down in q_forward:
        on_up.wait_recv()
        on_down.wait_recv()
        half = qa.at[at, :, :, k]
        q_cross.append((at, send(half, half, other_core)))

    line_receive(1)
    line_send(2)
    raw = jnp.zeros((PADDED, RANK), f32)
    for at, copy in q_cross:
        copy.wait_recv()
        columns = pl.ds(pl.multiple_of(at * (COLS // 2), COLS // 2), COLS // 2)
        raw = raw + dot(mb[:, columns], qa[at].reshape(COLS // 2, RANK), 1, 0)
    raw_b[...] = raw.astype(bf16)
    raw_rows = raw_b[...]

    gram = dot(raw_rows, raw_rows, 0, 0)
    gsend[0] = gram[:64]
    gsend[1] = gram[64:]
    gram_cross = send(gsend.at[1 - k], g1, other_core)

    raw_t = raw.T.astype(bf16)

    def image(half, part, store):
        columns = pl.ds(pl.multiple_of(half * (COLS // 2) + part * 256, 256), 256)
        block = dot(raw_t, mb[:, columns], 1, 0)
        store(part * 2, block[:, :128])
        store(part * 2 + 1, block[:, 128:])

    def store_far(at, block):
        rp[at] = block.astype(bf16)

    def store_near(at, block):
        rown[at] = block

    r_cross = []
    for chunk in (0, 1):
        for part in range(chunk * 4, chunk * 4 + 4):
            image(1 - k, part, store_far)
        piece = pl.ds(chunk * 8, 8)
        r_cross.append(send(rp.at[piece], r1.at[piece], other_core))

    gram_cross.wait_recv()
    g2[a] = gsend[k] + g1[...]
    gram_first = [send(g2.at[a], g2.at[a], first_axis(d)) for d in (2, 1, 3)]

    for part in range(8):
        image(k, part, store_near)

    for copy in r_cross:
        copy.wait_recv()
    r_first = []
    for d in (2, 1, 3):
        to = lax.rem(a + d, 4)
        for j in range(4):
            s1[d - 1, j] = (rown[to * 4 + j] + r1[to * 4 + j].astype(f32)).astype(bf16)
        r_first.append(send(s1.at[d - 1], r2.at[d - 1], first_axis(d)))

    for copy in gram_first:
        copy.wait_recv()
    g3[b] = (g2[0] + g2[1]) + (g2[2] + g2[3])
    gram_second = [send(g3.at[b], g3.at[b], second_axis(d)) for d in (2, 1, 3)]

    for copy in r_first:
        copy.wait_recv()
    for j in range(4):
        s2[j] = (rown[a * 4 + j] + r1[a * 4 + j].astype(f32)) + (
            (r2[0, j].astype(f32) + r2[1, j].astype(f32)) + r2[2, j].astype(f32)
        )
    r_second = []
    for d in (2, 1, 3):
        s2b[d - 1] = s2[lax.rem(b + d, 4)].astype(bf16)
        r_second.append(send(s2b.at[d - 1], r3.at[d - 1], second_axis(d)))

    for copy in gram_second:
        copy.wait_recv()
    g4[h] = (g3[0] + g3[1]) + (g3[2] + g3[3])
    gram_third = send(g4.at[h], g4.at[h], other_half)

    for copy in r_second:
        copy.wait_recv()
    s3b[...] = (
        s2[b] + ((r3[0].astype(f32) + r3[1].astype(f32)) + r3[2].astype(f32))
    ).astype(bf16)
    r_third = send(s3b, r4, other_half)

    gram_third.wait_recv()
    gfull[k] = g4[0] + g4[1]
    gram_last = send(gfull.at[k], gfull.at[k], other_core)
    gram_last.wait_recv()
    lower = inverse_lower(jnp.concatenate([gfull[0], gfull[1]], axis=0))

    r_third.wait_recv()
    image_sum = s3b[...].astype(f32) + r4[...].astype(f32)
    factor = dot(lower, image_sum, 1, 0, precise).astype(bf16)
    f_all[k, a, b, c] = factor
    squared = jnp.square(factor.astype(f32))
    nb[b, c] = dot(jnp.ones((8, RANK), f32), squared, 1, 1, precise)

    mine = f_all.at[k, a, b, c]
    square = nb.at[b, c]
    n_z = [send(square, square, along_z(d)) for d in (2, 1, 7)]
    z_copies = [send(mine, mine, along_z(d)) for d in (2, 1, 7)]
    basis = dot(raw_rows.astype(f32), lower, 1, 1, precise)[:OWN]
    p_all[c] = basis.astype(bf16)
    p_copies = [send(p_all.at[c], p_all.at[c], {"island": lax.rem(c + d, 4)}) for d in (1, 2, 3)]
    p_own[...] = (basis * (error_decay - 1.0)).astype(bf16)

    up_a, down_a = first_axis(1), first_axis(3)
    up_b, down_b = second_axis(1), second_axis(3)
    a_below, a_above, a_far = lax.rem(a + 3, 4), lax.rem(a + 1, 4), lax.rem(a + 2, 4)
    b_below, b_above, b_far = lax.rem(b + 3, 4), lax.rem(b + 1, 4), lax.rem(b + 2, 4)

    def ring_a(at):
        piece = f_all.at[k, a, at]
        return (at, send(piece, piece, up_a), send(piece, piece, down_a))

    def forward_a(ring):
        at, up, down = ring
        up.wait_recv()
        came = f_all.at[k, a_below, at, 0:2]
        on_up = send(came, came, up_a)
        down.wait_recv()
        came = f_all.at[k, a_above, at, 2:4]
        on_down = send(came, came, down_a)
        return (at, on_up, on_down)

    def cross(ring):
        at, on_up, on_down = ring
        on_up.wait_recv()
        on_down.wait_recv()
        part = f_all.at[k, :, at]
        return send(part, part, other_core)

    def finish(half, at):
        @pl.loop(0, 2)
        def _(pair):
            pieces = (pair * 2, pair * 2 + 1)
            every = [f_all[half, i, at].reshape(4 * RANK, 128) for i in pieces]
            mean = dot(p_scaled[...], jnp.concatenate(every, axis=1), 1, 0)
            own = [f_all[half, i, at, c] for i in pieces]
            decay = dot(p_own[...], jnp.concatenate(own, axis=1), 1, 0)
            for n, i in enumerate(pieces):
                lanes = slice(n * 128, n * 128 + 128)
                columns = pl.ds(
                    pl.multiple_of(half * (COLS // 2) + i * 512 + at * 128, 128), 128
                )
                matrix = grads_v[:, columns].astype(f32) + buffer_v[:, columns].astype(f32)
                buffer_new[:, columns] = (matrix + decay[:, lanes]).astype(bf16)
                means[...] = mean[:, lanes]
                carried = jnp.concatenate(
                    [mom_all[m, :, columns].astype(f32) for m in range(4)], axis=0
                )
                part = mean[:, lanes]
                anchor_new[:, columns] = (
                    anchor_v[:, columns].astype(f32)
                    - outer_rate * (part + outer_beta * (outer_beta * carried + part))
                ).astype(bf16)
                rows = pl.ds(pl.multiple_of(c * QUARTER, 8), QUARTER)
                momentum_new[:, columns] = outer_beta * mom_v[:, columns] + means[rows, :]

    for copy in n_z:
        copy.wait_recv()
    n_second = [send(nb.at[b], nb.at[b], second_axis(d)) for d in (2, 1, 3)]
    for copy in z_copies:
        copy.wait_recv()
    piece = f_all.at[k, a, b]
    up, down = send(piece, piece, up_b), send(piece, piece, down_b)
    ring_own = ring_a(b)
    line_receive(2)
    line_send(3)
    for copy in n_second:
        copy.wait_recv()
    na[a] = (nb[0] + nb[1]) + (nb[2] + nb[3])
    n_first = [send(na.at[a], na.at[a], first_axis(d)) for d in (2, 1, 3)]
    up.wait_recv()
    came = f_all.at[k, a, b_below, 0:2]
    on_up = send(came, came, up_b)
    down.wait_recv()
    came = f_all.at[k, a, b_above, 2:4]
    on_down = send(came, came, down_b)
    ring_below = ring_a(b_below)
    ring_above = ring_a(b_above)
    own_on = forward_a(ring_own)
    on_up.wait_recv()
    on_down.wait_recv()
    ring_far = ring_a(b_far)
    for copy in n_first:
        copy.wait_recv()
    nk[k] = (na[0] + na[1]) + (na[2] + na[3])
    n_cross = send(nk.at[k], nk.at[k], other_core)
    below_on = forward_a(ring_below)
    above_on = forward_a(ring_above)
    crossing = [cross(own_on)]
    far_on = forward_a(ring_far)
    crossing.append(cross(below_on))
    crossing.append(cross(above_on))
    n_cross.wait_recv()
    for copy in p_copies:
        copy.wait_recv()
    rate = math.sqrt(ROWS * COLS / RANK) / 4.0
    for island in range(4):
        total = (nk[0, island] + nk[1, island])[:1]
        scale = rate * lax.rsqrt(total + epsilon)
        p_scaled[:, island * RANK : (island + 1) * RANK] = (
            p_all[island].astype(f32) * scale
        ).astype(bf16)
    loads[3].wait()
    line_receive(3)
    finish(k, b)
    finish(k, b_below)
    finish(k, b_above)
    crossing.append(cross(far_on))
    for copy, at in zip(crossing, (a, a_below, a_above)):
        copy.wait_recv()
        finish(1 - k, at)
    finish(k, b_far)
    crossing[3].wait_recv()
    finish(1 - k, a_far)
    for copy in started:
        copy.wait_send()


def exchange(grads, buffer, q_old, anchor, momentum):
    vmem = pltpu.VMEM
    whole = pl.BlockSpec(memory_space=pltpu.VMEM)
    anywhere = pl.BlockSpec(memory_space=pltpu.HBM)
    block = (128, 128)
    return pl.pallas_call(
        exchange_kernel,
        out_shape=(
            vmem((OWN, COLS), bf16),
            vmem((OWN, COLS), bf16),
            vmem((QUARTER, COLS), f32),
        ),
        in_specs=[anywhere] * 5,
        out_specs=(whole, whole, whole),
        scratch_shapes=[
            vmem((2, 4, 4, 4, *block), bf16),
            vmem((OWN, 4 * RANK), bf16),
            vmem((OWN, RANK), bf16),
            vmem((4, QUARTER, COLS), bf16),
            vmem((OWN, COLS), bf16),
            vmem((OWN, 128), f32),
            vmem((4, 4, 8, 128), f32),
            vmem((4, 4, 8, 128), f32),
            vmem((2, 4, 8, 128), f32),
            vmem((64, RANK), f32),
            vmem((OWN, COLS), bf16),
            vmem((OWN, COLS), bf16),
            vmem((QUARTER, COLS), f32),
            vmem((PADDED, COLS), bf16),
            vmem((2, 4, 4, 2, 64, RANK), bf16),
            vmem((PADDED, RANK), bf16),
            vmem((2, 64, 128), f32),
            vmem((64, 128), f32),
            vmem((4, 64, 128), f32),
            vmem((4, 64, 128), f32),
            vmem((2, 64, 128), f32),
            vmem((2, 64, 128), f32),
            vmem((16, *block), bf16),
            vmem((16, *block), f32),
            vmem((16, *block), bf16),
            vmem((3, 4, *block), bf16),
            vmem((3, 4, *block), bf16),
            vmem((4, *block), f32),
            vmem((3, *block), bf16),
            vmem((3, *block), bf16),
            vmem(block, bf16),
            vmem(block, bf16),
            vmem((4, OWN, RANK), bf16),
            pltpu.SemaphoreType.DMA((5,)),
            pltpu.SemaphoreType.DMA((96,)),
            pltpu.SemaphoreType.DMA((96,)),
        ],
        compiler_params=pltpu.CompilerParams(
            collective_id=0, has_side_effects=True, vmem_limit_bytes=36 * 1024 * 1024
        ),
        name="exchange",
    )(*(pltpu.with_memory_space_constraint(v, pltpu.HBM) for v in (grads, buffer, q_old, anchor, momentum)))


def body(grads, buffer, q_old, anchor, momentum):
    anchor_new, buffer_new, momentum_new = exchange(
        grads[0, 0], buffer[0], q_old[0], anchor, momentum
    )
    return (anchor_new, buffer_new[None], momentum_new)


def solution(mesh):
    split = Mesh(
        mesh.devices.reshape(mesh.shape["island"], 2, 4, 4, 2),
        ("island", "fsdp_0", "fsdp_1", "fsdp_2", "fsdp_3"),
    )
    return jax.shard_map(
        body,
        mesh=split,
        in_specs=(
            P("island", None, FSDP, None),
            P("island", FSDP, None),
            P("island", FSDP, None),
            P(FSDP, None),
            P(FSDP_ISLAND, None),
        ),
        out_specs=(P(FSDP, None), P("island", FSDP, None), P(FSDP_ISLAND, None)),
        check_vma=False,
    )
```

```python
import math

import jax
import jax.numpy as jnp
from jax import lax
from jax.experimental import pallas as pl
from jax.experimental.pallas import tpu as pltpu
from jax.sharding import Mesh
from jax.sharding import PartitionSpec as P

ROWS = 14336
COLS = 4096
RANK = 128
FSDP = ("fsdp_0", "fsdp_1", "fsdp_2", "fsdp_3")
FSDP_ISLAND = ("fsdp_0", "fsdp_1", "fsdp_2", "fsdp_3", "island")
OWN = 224
PADDED = 256
QUARTER = 56
MESH = pl.DeviceIdType.MESH

precise = lax.Precision.HIGHEST
error_decay = 0.95
outer_beta = 0.9
outer_rate = 0.7
epsilon = 1e-06
f32 = jnp.float32
bf16 = jnp.bfloat16


def dot(left, right, left_dim, right_dim, precision=None):
    return lax.dot_general(
        left,
        right,
        (((left_dim,), (right_dim,)), ((), ())),
        precision=precision,
        preferred_element_type=f32,
    )


def inverse_lower(gram, width=8):
    n = gram.shape[0]
    rest = gram
    side = (
        lax.broadcasted_iota(jnp.int32, (n, n), 0) == lax.broadcasted_iota(jnp.int32, (n, n), 1)
    ).astype(f32)
    done = []
    for first in range(0, n, 8):
        rows = lax.broadcasted_iota(jnp.int32, rest.shape, 0)
        scale = jnp.ones((8, n), f32)
        head = lax.broadcasted_iota(jnp.int32, (8, n), 0)
        for at in range(0, 8, width):
            columns = [
                jnp.broadcast_to(rest[:, first + at + i : first + at + i + 1], rest.shape)
                for i in range(width)
            ]
            for i in range(width):
                row = at + i
                pivot = columns[i][row : row + 1, :]
                times = jnp.where(rows > row, columns[i] * (1.0 / pivot), 0.0)
                scale = jnp.where(head == row, pivot, scale)
                for j in range(i + 1, width):
                    columns[j] = columns[j] - times * columns[j][row : row + 1, :]
                rest = rest - times * rest[row : row + 1, :]
                side = side - times * side[row : row + 1, :]
        done.append(side[:8] * lax.rsqrt(scale))
        rest, side = rest[8:], side[8:]
    return jnp.concatenate(done, axis=0)


def exchange_kernel(
    grads,
    buffer,
    q_old,
    anchor,
    momentum,
    anchor_new,
    buffer_new,
    momentum_new,
    f_all,
    p_scaled,
    p_own,
    mom_all,
    anchor_v,
    means,
    nb,
    na,
    nk,
    q_v,
    grads_v,
    buffer_v,
    mom_v,
    mb,
    mp,
    qa,
    raw_b,
    gsend,
    g1,
    g2,
    g3,
    g4,
    gfull,
    rp,
    rown,
    r1,
    s1,
    r2,
    s2,
    s2b,
    r3,
    s3b,
    r4,
    p_all,
    load_sem,
    send_sem,
    recv_sem,
):
    c = lax.axis_index("island")
    h = lax.axis_index("fsdp_0")
    x = lax.axis_index("fsdp_1")
    y = lax.axis_index("fsdp_2")
    k = lax.axis_index("fsdp_3")
    z = h * 4 + c
    a = x * (1 - k) + y * k
    b = y * (1 - k) + x * k

    def first_axis(d):
        return {"fsdp_1": lax.rem(x + d * (1 - k), 4), "fsdp_2": lax.rem(y + d * k, 4)}

    def second_axis(d):
        return {"fsdp_1": lax.rem(x + d * k, 4), "fsdp_2": lax.rem(y + d * (1 - k), 4)}

    def along_z(d):
        to = lax.rem(z + d, 8)
        return {"fsdp_0": to // 4, "island": lax.rem(to, 4)}

    other_core = {"fsdp_3": 1 - k}
    other_half = {"fsdp_0": 1 - h}

    peers = [other_core, other_half]
    for d in (1, 2, 3):
        peers.append({"fsdp_1": lax.rem(x + d, 4)})
        peers.append({"fsdp_2": lax.rem(y + d, 4)})
        peers.append({"island": lax.rem(c + d, 4)})
    for d in (1, 2, 6, 7):
        peers.append(along_z(d))

    counter = [0]
    started = []

    def copy_to(src, dst, device):
        at = counter[0]
        counter[0] += 1
        copy = pltpu.make_async_remote_copy(
            src_ref=src,
            dst_ref=dst,
            send_sem=send_sem.at[at],
            recv_sem=recv_sem.at[at],
            device_id=device,
            device_id_type=MESH,
        )
        return copy

    def send(src, dst, device):
        copy = copy_to(src, dst, device)
        copy.start()
        started.append(copy)
        return copy

    barrier = pltpu.get_barrier_semaphore()
    for peer in peers:
        pl.semaphore_signal(barrier, inc=1, device_id=peer, device_id_type=MESH)

    loads = [
        pltpu.make_async_copy(momentum, mom_v, load_sem.at[0]),
        pltpu.make_async_copy(grads, grads_v, load_sem.at[1]),
        pltpu.make_async_copy(buffer, buffer_v, load_sem.at[2]),
        pltpu.make_async_copy(anchor, anchor_v, load_sem.at[3]),
        pltpu.make_async_copy(q_old, q_v, load_sem.at[4]),
    ]
    for at in (4, 0, 1, 2, 3):
        loads[at].start()
    loads[4].wait()
    qa[h, k, a, b] = q_v[...].astype(bf16)
    pl.semaphore_wait(barrier, len(peers))

    own_piece = qa.at[h, k, a, b]
    far_piece = qa.at[1 - h, k, a, b]
    q_far = send(own_piece, own_piece, other_half)
    q_first = [send(own_piece, own_piece, first_axis(d)) for d in (2, 1, 3)]

    line = []
    for step, first, rows in ((1, 0, 56), (2, 0, 56), (3, 0, 32), (3, 32, 24)):
        up_ok = jnp.logical_and(c < 3, c >= step - 1)
        down_ok = jnp.logical_and(c > 0, c + step - 1 <= 3)
        up_part = mom_all.at[lax.rem(c - (step - 1) + 4, 4), pl.ds(first, rows)]
        down_part = mom_all.at[lax.rem(c + (step - 1), 4), pl.ds(first, rows)]
        up = copy_to(up_part, up_part, {"island": lax.rem(c + 1, 4)})
        down = copy_to(down_part, down_part, {"island": lax.rem(c + 3, 4)})
        line.append((up_ok, up, c - step >= 0, down_ok, down, c + step <= 3))

    def line_send(hop):
        up_ok, up, _, down_ok, down, _ = line[hop]

        @pl.when(up_ok)
        def _():
            up.start()

        @pl.when(down_ok)
        def _():
            down.start()

    def line_receive(hop):
        up_ok, up, from_below, down_ok, down, from_above = line[hop]

        @pl.when(from_below)
        def _():
            up.wait_recv()

        @pl.when(from_above)
        def _():
            down.wait_recv()

        @pl.when(up_ok)
        def _():
            up.wait_send()

        @pl.when(down_ok)
        def _():
            down.wait_send()

    loads[0].wait()
    mom_all[c] = mom_v[...].astype(bf16)
    line_send(0)

    loads[1].wait()
    loads[2].wait()

    low_lanes = lax.broadcasted_iota(jnp.int32, (16, 128), 1) < 64

    @pl.loop(0, OWN // 16)
    def _(i):
        at = pl.ds(pl.multiple_of(i * 16, 16), 16)
        matrix = grads_v[at, :].astype(f32) + buffer_v[at, :].astype(f32)
        mb[at, :] = matrix.astype(bf16)

        def block(half, row, column):
            first = (half * 16 + row * 4 + column) * 128
            return matrix[:, first : first + 128]

        for half in (0, 1):
            for outer in range(4):
                for pair in (0, 1):
                    lanes = slice((outer * 2 + pair) * 128, (outer * 2 + pair + 1) * 128)
                    one, two = block(half, outer, pair * 2), block(half, outer, pair * 2 + 1)
                    mp[half, 0, at, lanes] = jnp.where(
                        low_lanes, one, pltpu.roll(two, 64, 1)
                    ).astype(bf16)
                    one, two = block(half, pair * 2, outer), block(half, pair * 2 + 1, outer)
                    mp[half, 1, at, lanes] = jnp.where(
                        low_lanes, pltpu.roll(one, 64, 1), two
                    ).astype(bf16)

    mb[OWN:, :] = jnp.zeros((PADDED - OWN, COLS), bf16)
    for half in (0, 1):
        for core in (0, 1):
            mp[half, core, OWN:, :] = jnp.zeros((PADDED - OWN, COLS // 4), bf16)

    def gathered(at, copies):
        for copy in copies:
            copy.wait_recv()
        mine = qa.at[at, k, :, b]
        return (at, [send(mine, mine, second_axis(d)) for d in (2, 1, 3)])

    q_second = [gathered(h, q_first)]
    q_far.wait_recv()
    q_first = [send(far_piece, far_piece, first_axis(d)) for d in (2, 1, 3)]
    q_second.append(gathered(1 - h, q_first))
    q_cross = []
    for at, copies in q_second:
        for copy in copies:
            copy.wait_recv()
        half = qa.at[at, k]
        q_cross.append((at, send(half, half, other_core)))

    line_receive(0)
    line_send(1)
    raw = jnp.zeros((PADDED, RANK), f32)
    for at, copy in q_cross:
        raw = raw + dot(mp[at, k], qa[at, k].reshape(COLS // 4, RANK), 1, 0)
        copy.wait_recv()
        raw = raw + dot(mp[at, 1 - k], qa[at, 1 - k].reshape(COLS // 4, RANK), 1, 0)
    raw_b[...] = raw.astype(bf16)
    raw_rows = raw_b[...]

    gram = dot(raw_rows, raw_rows, 0, 0)
    gsend[0] = gram[:64]
    gsend[1] = gram[64:]
    gram_cross = send(gsend.at[1 - k], g1, other_core)

    raw_t = raw.T.astype(bf16)

    def image(half, part, store):
        columns = pl.ds(pl.multiple_of(half * (COLS // 2) + part * 256, 256), 256)
        block = dot(raw_t, mb[:, columns], 1, 0)
        store(part * 2, block[:, :128])
        store(part * 2 + 1, block[:, 128:])

    def store_far(at, block):
        rp[at] = block.astype(bf16)

    def store_near(at, block):
        rown[at] = block

    r_cross = []
    for chunk in (0, 1):
        for part in range(chunk * 4, chunk * 4 + 4):
            image(1 - k, part, store_far)
        piece = pl.ds(chunk * 8, 8)
        r_cross.append(send(rp.at[piece], r1.at[piece], other_core))

    gram_cross.wait_recv()
    g2[a] = gsend[k] + g1[...]
    gram_first = [send(g2.at[a], g2.at[a], first_axis(d)) for d in (2, 1, 3)]

    for part in range(8):
        image(k, part, store_near)

    for copy in r_cross:
        copy.wait_recv()
    r_first = []
    for d in (2, 1, 3):
        to = lax.rem(a + d, 4)
        for j in range(4):
            s1[d - 1, j] = (rown[to * 4 + j] + r1[to * 4 + j].astype(f32)).astype(bf16)
        r_first.append(send(s1.at[d - 1], r2.at[d - 1], first_axis(d)))

    for copy in gram_first:
        copy.wait_recv()
    g3[b] = (g2[0] + g2[1]) + (g2[2] + g2[3])
    gram_second = [send(g3.at[b], g3.at[b], second_axis(d)) for d in (2, 1, 3)]

    for copy in r_first:
        copy.wait_recv()
    for j in range(4):
        s2[j] = (rown[a * 4 + j] + r1[a * 4 + j].astype(f32)) + (
            (r2[0, j].astype(f32) + r2[1, j].astype(f32)) + r2[2, j].astype(f32)
        )
    r_second = []
    for d in (2, 1, 3):
        s2b[d - 1] = s2[lax.rem(b + d, 4)].astype(bf16)
        r_second.append(send(s2b.at[d - 1], r3.at[d - 1], second_axis(d)))

    for copy in gram_second:
        copy.wait_recv()
    g4[h] = (g3[0] + g3[1]) + (g3[2] + g3[3])
    gram_third = send(g4.at[h], g4.at[h], other_half)

    for copy in r_second:
        copy.wait_recv()
    s3b[...] = (
        s2[b] + ((r3[0].astype(f32) + r3[1].astype(f32)) + r3[2].astype(f32))
    ).astype(bf16)
    r_third = send(s3b, r4, other_half)
    line_receive(1)
    line_send(2)

    gram_third.wait_recv()
    gfull[k] = g4[0] + g4[1]
    gram_last = send(gfull.at[k], gfull.at[k], other_core)
    gram_last.wait_recv()
    lower = inverse_lower(jnp.concatenate([gfull[0], gfull[1]], axis=0))

    r_third.wait_recv()
    image_sum = s3b[...].astype(f32) + r4[...].astype(f32)
    factor = dot(lower, image_sum, 1, 0, precise).astype(bf16)
    f_all[k, a, b, 0] = factor
    squared = jnp.square(factor.astype(f32))
    nb[b, c] = dot(jnp.ones((8, RANK), f32), squared, 1, 1, precise)

    square = nb.at[b, c]
    n_z = [send(square, square, along_z(d)) for d in (2, 1, 7)]
    z_copies = []
    for d, rows in ((2, pl.ds(0, 64)), (6, pl.ds(64, 64)), (1, pl.ds(0, 128)), (7, pl.ds(0, 128))):
        mine = f_all.at[k, a, b, 0, rows]
        z_copies.append(send(mine, f_all.at[k, a, b, (-d) % 4, rows], along_z(d)))

    up_a, down_a = first_axis(1), first_axis(3)
    up_b, down_b = second_axis(1), second_axis(3)
    a_below, a_above, a_far = lax.rem(a + 3, 4), lax.rem(a + 1, 4), lax.rem(a + 2, 4)
    b_below, b_above, b_far = lax.rem(b + 3, 4), lax.rem(b + 1, 4), lax.rem(b + 2, 4)

    def pass_on(at, islands, *devices):
        part = f_all.at[k, at[0], at[1], pl.ds(islands[0], islands[1] - islands[0])]
        return [send(part, part, device) for device in devices]

    early_b = pass_on((a, b), (0, 1), up_b, down_b)
    early_a = pass_on((a, b), (0, 1), up_a, down_a)
    basis = dot(raw_rows.astype(f32), lower, 1, 1, precise)[:OWN]
    p_all[c] = basis.astype(bf16)
    p_copies = [send(p_all.at[c], p_all.at[c], {"island": lax.rem(c + d, 4)}) for d in (1, 2, 3)]
    p_own[...] = (basis * (error_decay - 1.0)).astype(bf16)

    order = [lax.rem(m - c + 4, 4) for m in range(4)]

    def finish(half, at):
        for pair in (0, 1):
            pieces = (pair * 2, pair * 2 + 1)
            every = [
                jnp.concatenate([f_all[half, i, at, order[m]] for m in range(4)], axis=0)
                for i in pieces
            ]
            mean = dot(p_scaled[...], jnp.concatenate(every, axis=1), 1, 0)
            own = [f_all[half, i, at, 0] for i in pieces]
            decay = dot(p_own[...], jnp.concatenate(own, axis=1), 1, 0)
            for n, i in enumerate(pieces):
                lanes = slice(n * 128, n * 128 + 128)
                columns = pl.ds(
                    pl.multiple_of(half * (COLS // 2) + i * 512 + at * 128, 128), 128
                )
                matrix = grads_v[:, columns].astype(f32) + buffer_v[:, columns].astype(f32)
                buffer_new[:, columns] = (matrix + decay[:, lanes]).astype(bf16)
                means[...] = mean[:, lanes]
                carried = jnp.concatenate(
                    [mom_all[m, :, columns].astype(f32) for m in range(4)], axis=0
                )
                part = mean[:, lanes]
                anchor_new[:, columns] = (
                    anchor_v[:, columns].astype(f32)
                    - outer_rate * (part + outer_beta * (outer_beta * carried + part))
                ).astype(bf16)
                rows = pl.ds(pl.multiple_of(c * QUARTER, 8), QUARTER)
                momentum_new[:, columns] = outer_beta * mom_v[:, columns] + means[rows, :]

    for copy in early_b:
        copy.wait_recv()
    early_b_on = pass_on((a, b_above), (0, 1), down_b)
    early_below = pass_on((a, b_below), (0, 1), up_a, down_a)
    early_above = pass_on((a, b_above), (0, 1), up_a, down_a)
    for copy in early_a:
        copy.wait_recv()
    early_a_on = pass_on((a_above, b), (0, 1), down_a)

    for copy in n_z:
        copy.wait_recv()
    n_second = [send(nb.at[b], nb.at[b], second_axis(d)) for d in (2, 1, 3)]
    for copy in z_copies:
        copy.wait_recv()
    up_copy, down_copy = pass_on((a, b), (1, 4), up_b, down_b)
    own_up, own_down = pass_on((a, b), (1, 4), up_a, down_a)
    line_send(3)
    for copy in n_second:
        copy.wait_recv()
    na[a] = (nb[0] + nb[1]) + (nb[2] + nb[3])
    n_first = [send(na.at[a], na.at[a], first_axis(d)) for d in (2, 1, 3)]
    up_copy.wait_recv()
    b_on = pass_on((a, b_below), (2, 4), up_b)
    down_copy.wait_recv()
    b_on += pass_on((a, b_above), (1, 2), down_b)
    below_up, below_down = pass_on((a, b_below), (1, 4), up_a, down_a)
    above_up, above_down = pass_on((a, b_above), (1, 4), up_a, down_a)
    own_up.wait_recv()
    own_on = pass_on((a_below, b), (2, 4), up_a)
    own_down.wait_recv()
    own_on += pass_on((a_above, b), (1, 2), down_a)
    for copy in early_b_on + b_on:
        copy.wait_recv()
    far_up, far_down = pass_on((a, b_far), (0, 4), up_a, down_a)
    for copy in n_first:
        copy.wait_recv()
    nk[k] = (na[0] + na[1]) + (na[2] + na[3])
    n_cross = send(nk.at[k], nk.at[k], other_core)

    def forward_a(at, early, up, down):
        for copy in early:
            copy.wait_recv()
        up.wait_recv()
        on = pass_on((a_below, at), (2, 4), up_a)
        down.wait_recv()
        return on + pass_on((a_above, at), (0, 2), down_a)

    def cross(at, arriving):
        for copy in arriving:
            copy.wait_recv()
        part = f_all.at[k, :, at]
        return send(part, part, other_core)

    below_on = forward_a(b_below, early_below, below_up, below_down)
    above_on = forward_a(b_above, early_above, above_up, above_down)
    crossing = [cross(b, early_a_on + own_on)]
    n_cross.wait_recv()
    for copy in p_copies:
        copy.wait_recv()
    rate = math.sqrt(ROWS * COLS / RANK) / 4.0
    for island in range(4):
        total = (nk[0, island] + nk[1, island])[:1]
        scale = rate * lax.rsqrt(total + epsilon)
        p_scaled[:, island * RANK : (island + 1) * RANK] = (
            p_all[island].astype(f32) * scale
        ).astype(bf16)
    loads[3].wait()
    far_on = forward_a(b_far, [], far_up, far_down)
    line_receive(2)
    line_receive(3)
    finish(k, b)
    crossing.append(cross(b_below, below_on))
    crossing.append(cross(b_above, above_on))
    crossing[0].wait_recv()
    finish(1 - k, a)
    finish(k, b_below)
    crossing.append(cross(b_far, far_on))
    for copy, at in zip(crossing[1:3], (a_below, a_above)):
        copy.wait_recv()
        finish(1 - k, at)
    finish(k, b_above)
    finish(k, b_far)
    crossing[3].wait_recv()
    finish(1 - k, a_far)
    for copy in started:
        copy.wait_send()


def exchange(grads, buffer, q_old, anchor, momentum):
    vmem = pltpu.VMEM
    whole = pl.BlockSpec(memory_space=pltpu.VMEM)
    anywhere = pl.BlockSpec(memory_space=pltpu.HBM)
    block = (128, 128)
    return pl.pallas_call(
        exchange_kernel,
        out_shape=(
            vmem((OWN, COLS), bf16),
            vmem((OWN, COLS), bf16),
            vmem((QUARTER, COLS), f32),
        ),
        in_specs=[anywhere] * 5,
        out_specs=(whole, whole, whole),
        scratch_shapes=[
            vmem((2, 4, 4, 4, *block), bf16),
            vmem((OWN, 4 * RANK), bf16),
            vmem((OWN, RANK), bf16),
            vmem((4, QUARTER, COLS), bf16),
            vmem((OWN, COLS), bf16),
            vmem((OWN, 128), f32),
            vmem((4, 4, 8, 128), f32),
            vmem((4, 4, 8, 128), f32),
            vmem((2, 4, 8, 128), f32),
            vmem((64, RANK), f32),
            vmem((OWN, COLS), bf16),
            vmem((OWN, COLS), bf16),
            vmem((QUARTER, COLS), f32),
            vmem((PADDED, COLS), bf16),
            vmem((2, 2, PADDED, COLS // 4), bf16),
            vmem((2, 2, 4, 4, 64, RANK), bf16),
            vmem((PADDED, RANK), bf16),
            vmem((2, 64, 128), f32),
            vmem((64, 128), f32),
            vmem((4, 64, 128), f32),
            vmem((4, 64, 128), f32),
            vmem((2, 64, 128), f32),
            vmem((2, 64, 128), f32),
            vmem((16, *block), bf16),
            vmem((16, *block), f32),
            vmem((16, *block), bf16),
            vmem((3, 4, *block), bf16),
            vmem((3, 4, *block), bf16),
            vmem((4, *block), f32),
            vmem((3, *block), bf16),
            vmem((3, *block), bf16),
            vmem(block, bf16),
            vmem(block, bf16),
            vmem((4, OWN, RANK), bf16),
            pltpu.SemaphoreType.DMA((5,)),
            pltpu.SemaphoreType.DMA((128,)),
            pltpu.SemaphoreType.DMA((128,)),
        ],
        compiler_params=pltpu.CompilerParams(
            collective_id=0, has_side_effects=True, vmem_limit_bytes=36 * 1024 * 1024
        ),
        name="exchange",
    )(*(pltpu.with_memory_space_constraint(v, pltpu.HBM) for v in (grads, buffer, q_old, anchor, momentum)))


def store_kernel(anchor_v, buffer_v, momentum_v, anchor_new, buffer_new, momentum_new, sems):
    copies = []
    for source, target, parts in (
        (anchor_v, anchor_new, 4),
        (buffer_v, buffer_new, 4),
        (momentum_v, momentum_new, 1),
    ):
        height = source.shape[0] // parts
        for part in range(parts):
            rows = pl.ds(part * height, height)
            copy = pltpu.make_async_copy(source.at[rows], target.at[rows], sems.at[len(copies)])
            copy.start()
            copies.append(copy)
    for copy in copies:
        copy.wait()


def store(anchor_new, buffer_new, momentum_new):
    return pl.pallas_call(
        store_kernel,
        out_shape=(
            jax.ShapeDtypeStruct((OWN, COLS), bf16),
            jax.ShapeDtypeStruct((OWN, COLS), bf16),
            jax.ShapeDtypeStruct((QUARTER, COLS), f32),
        ),
        in_specs=[pl.BlockSpec(memory_space=pltpu.VMEM)] * 3,
        out_specs=[pl.BlockSpec(memory_space=pltpu.HBM)] * 3,
        scratch_shapes=[pltpu.SemaphoreType.DMA((9,))],
        compiler_params=pltpu.CompilerParams(vmem_limit_bytes=1024 * 1024),
        name="store",
    )(anchor_new, buffer_new, momentum_new)


def body(grads, buffer, q_old, anchor, momentum):
    anchor_new, buffer_new, momentum_new = store(
        *exchange(grads[0, 0], buffer[0], q_old[0], anchor, momentum)
    )
    return (anchor_new, buffer_new[None], momentum_new)


def solution(mesh):
    split = Mesh(
        mesh.devices.reshape(mesh.shape["island"], 2, 4, 4, 2),
        ("island", "fsdp_0", "fsdp_1", "fsdp_2", "fsdp_3"),
    )
    return jax.shard_map(
        body,
        mesh=split,
        in_specs=(
            P("island", None, FSDP, None),
            P("island", FSDP, None),
            P("island", FSDP, None),
            P(FSDP, None),
            P(FSDP_ISLAND, None),
        ),
        out_specs=(P(FSDP, None), P("island", FSDP, None), P(FSDP_ISLAND, None)),
        check_vma=False,
    )
```

```python
import math

import jax
import jax.numpy as jnp
from jax import lax
from jax.experimental import pallas as pl
from jax.experimental.pallas import tpu as pltpu
from jax.sharding import Mesh
from jax.sharding import PartitionSpec as P

ROWS = 14336
COLS = 4096
RANK = 128
FSDP = ("fsdp_0", "fsdp_1", "fsdp_2", "fsdp_3")
FSDP_ISLAND = ("fsdp_0", "fsdp_1", "fsdp_2", "fsdp_3", "island")
OWN = 224
PADDED = 256
QUARTER = 56
MESH = pl.DeviceIdType.MESH

precise = lax.Precision.HIGHEST
error_decay = 0.95
outer_beta = 0.9
outer_rate = 0.7
epsilon = 1e-06
f32 = jnp.float32
bf16 = jnp.bfloat16


def dot(left, right, left_dim, right_dim, precision=None):
    return lax.dot_general(
        left,
        right,
        (((left_dim,), (right_dim,)), ((), ())),
        precision=precision,
        preferred_element_type=f32,
    )


def inverse_lower(gram, width=8):
    n = gram.shape[0]
    rest = gram
    side = (
        lax.broadcasted_iota(jnp.int32, (n, n), 0) == lax.broadcasted_iota(jnp.int32, (n, n), 1)
    ).astype(f32)
    done = []
    for first in range(0, n, 8):
        rows = lax.broadcasted_iota(jnp.int32, rest.shape, 0)
        scale = jnp.ones((8, n), f32)
        head = lax.broadcasted_iota(jnp.int32, (8, n), 0)
        for at in range(0, 8, width):
            columns = [
                jnp.broadcast_to(rest[:, first + at + i : first + at + i + 1], rest.shape)
                for i in range(width)
            ]
            for i in range(width):
                row = at + i
                pivot = columns[i][row : row + 1, :]
                times = jnp.where(rows > row, columns[i] * (1.0 / pivot), 0.0)
                scale = jnp.where(head == row, pivot, scale)
                for j in range(i + 1, width):
                    columns[j] = columns[j] - times * columns[j][row : row + 1, :]
                rest = rest - times * rest[row : row + 1, :]
                side = side - times * side[row : row + 1, :]
        done.append(side[:8] * lax.rsqrt(scale))
        rest, side = rest[8:], side[8:]
    return jnp.concatenate(done, axis=0)


def exchange_kernel(
    grads,
    buffer,
    q_old,
    anchor,
    momentum,
    anchor_new,
    buffer_new,
    momentum_new,
    f_all,
    p_scaled,
    p_own,
    mom_all,
    anchor_v,
    means,
    nb,
    na,
    nk,
    q_v,
    grads_v,
    buffer_v,
    mom_v,
    mb,
    mp,
    qa,
    raw_b,
    gsend,
    g1,
    g2,
    g3,
    g4,
    gfull,
    rp,
    rown,
    r1,
    s1,
    r2,
    s2,
    s2b,
    r3,
    s3b,
    r4,
    p_all,
    load_sem,
    send_sem,
    recv_sem,
):
    c = lax.axis_index("island")
    h = lax.axis_index("fsdp_0")
    x = lax.axis_index("fsdp_1")
    y = lax.axis_index("fsdp_2")
    k = lax.axis_index("fsdp_3")
    z = h * 4 + c
    a = x * (1 - k) + y * k
    b = y * (1 - k) + x * k

    def first_axis(d):
        return {"fsdp_1": lax.rem(x + d * (1 - k), 4), "fsdp_2": lax.rem(y + d * k, 4)}

    def second_axis(d):
        return {"fsdp_1": lax.rem(x + d * k, 4), "fsdp_2": lax.rem(y + d * (1 - k), 4)}

    def along_z(d):
        to = lax.rem(z + d, 8)
        return {"fsdp_0": to // 4, "island": lax.rem(to, 4)}

    other_core = {"fsdp_3": 1 - k}
    other_half = {"fsdp_0": 1 - h}

    peers = [other_core, other_half]
    for d in (1, 2, 3):
        peers.append({"fsdp_1": lax.rem(x + d, 4)})
        peers.append({"fsdp_2": lax.rem(y + d, 4)})
        peers.append({"island": lax.rem(c + d, 4)})
    for d in (1, 2, 6, 7):
        peers.append(along_z(d))

    counter = [0]
    started = []

    def copy_to(src, dst, device):
        at = counter[0]
        counter[0] += 1
        copy = pltpu.make_async_remote_copy(
            src_ref=src,
            dst_ref=dst,
            send_sem=send_sem.at[at],
            recv_sem=recv_sem.at[at],
            device_id=device,
            device_id_type=MESH,
        )
        return copy

    def send(src, dst, device):
        copy = copy_to(src, dst, device)
        copy.start()
        started.append(copy)
        return copy

    barrier = pltpu.get_barrier_semaphore()
    for peer in peers:
        pl.semaphore_signal(barrier, inc=1, device_id=peer, device_id_type=MESH)

    loads = [
        pltpu.make_async_copy(momentum, mom_v, load_sem.at[0]),
        pltpu.make_async_copy(grads, grads_v, load_sem.at[1]),
        pltpu.make_async_copy(buffer, buffer_v, load_sem.at[2]),
        pltpu.make_async_copy(anchor, anchor_v, load_sem.at[3]),
        pltpu.make_async_copy(q_old, q_v, load_sem.at[4]),
    ]
    for at in (4, 0, 1, 2, 3):
        loads[at].start()
    loads[4].wait()
    qa[h, k, a, b] = q_v[...].astype(bf16)
    pl.semaphore_wait(barrier, len(peers))

    def along_second(part):
        return [send(part, part, second_axis(d)) for d in (2, 1, 3)]

    def first_sends(part):
        return {d: send(part, part, first_axis(d)) for d in (2, 1, 3)}

    own_piece = qa.at[h, k, a, b]
    far_piece = qa.at[1 - h, k, a, b]
    q_far = send(own_piece, own_piece, other_half)
    q_first = first_sends(own_piece)
    on_near = along_second(own_piece)

    line = []
    for step, first, rows in ((1, 0, 56), (2, 0, 40), (2, 40, 16), (3, 0, 24), (3, 24, 32)):
        up_ok = jnp.logical_and(c < 3, c >= step - 1)
        down_ok = jnp.logical_and(c > 0, c + step - 1 <= 3)
        up_part = mom_all.at[lax.rem(c - (step - 1) + 4, 4), pl.ds(first, rows)]
        down_part = mom_all.at[lax.rem(c + (step - 1), 4), pl.ds(first, rows)]
        up = copy_to(up_part, up_part, {"island": lax.rem(c + 1, 4)})
        down = copy_to(down_part, down_part, {"island": lax.rem(c + 3, 4)})
        line.append((up_ok, up, c - step >= 0, down_ok, down, c + step <= 3))

    def line_send(hop):
        up_ok, up, _, down_ok, down, _ = line[hop]

        @pl.when(up_ok)
        def _():
            up.start()

        @pl.when(down_ok)
        def _():
            down.start()

    def line_receive(hop):
        up_ok, up, from_below, down_ok, down, from_above = line[hop]

        @pl.when(from_below)
        def _():
            up.wait_recv()

        @pl.when(from_above)
        def _():
            down.wait_recv()

        @pl.when(up_ok)
        def _():
            up.wait_send()

        @pl.when(down_ok)
        def _():
            down.wait_send()

    loads[0].wait()
    mom_all[c] = mom_v[...].astype(bf16)
    line_send(0)

    loads[1].wait()
    loads[2].wait()

    low_lanes = lax.broadcasted_iota(jnp.int32, (16, 128), 1) < 64

    @pl.loop(0, OWN // 16)
    def _(i):
        at = pl.ds(pl.multiple_of(i * 16, 16), 16)
        matrix = grads_v[at, :].astype(f32) + buffer_v[at, :].astype(f32)
        mb[at, :] = matrix.astype(bf16)

        def block(half, row, column):
            first = (half * 16 + row * 4 + column) * 128
            return matrix[:, first : first + 128]

        for half in (0, 1):
            for outer in range(4):
                for pair in (0, 1):
                    lanes = slice((outer * 2 + pair) * 128, (outer * 2 + pair + 1) * 128)
                    one, two = block(half, outer, pair * 2), block(half, outer, pair * 2 + 1)
                    mp[half, 0, at, lanes] = jnp.where(
                        low_lanes, one, pltpu.roll(two, 64, 1)
                    ).astype(bf16)
                    one, two = block(half, pair * 2, outer), block(half, pair * 2 + 1, outer)
                    mp[half, 1, at, lanes] = jnp.where(
                        low_lanes, pltpu.roll(one, 64, 1), two
                    ).astype(bf16)

    mb[OWN:, :] = jnp.zeros((PADDED - OWN, COLS), bf16)
    for half in (0, 1):
        for core in (0, 1):
            mp[half, core, OWN:, :] = jnp.zeros((PADDED - OWN, COLS // 4), bf16)

    def arrived(at, copies):
        on = []
        for d in (1, 3, 2):
            copies[d].wait_recv()
            on += along_second(qa.at[at, k, lax.rem(a + 4 - d, 4), b])
        return on

    on_near += arrived(h, q_first)
    q_far.wait_recv()
    q_first = first_sends(far_piece)
    on_far = along_second(far_piece)
    on_far += arrived(1 - h, q_first)
    q_second = [(h, on_near), (1 - h, on_far)]
    q_cross = []
    for at, copies in q_second:
        for copy in copies:
            copy.wait_recv()
        half = qa.at[at, k]
        q_cross.append((at, send(half, half, other_core)))

    line_receive(0)
    line_send(1)
    raw = jnp.zeros((PADDED, RANK), f32)
    for at, copy in q_cross:
        raw = raw + dot(mp[at, k], qa[at, k].reshape(COLS // 4, RANK), 1, 0)
        copy.wait_recv()
        raw = raw + dot(mp[at, 1 - k], qa[at, 1 - k].reshape(COLS // 4, RANK), 1, 0)
    raw_b[...] = raw.astype(bf16)
    raw_rows = raw_b[...]

    def total_of(parts):
        one, two, three, four = (parts[i].astype(f32) for i in range(4))
        return (one + two) + (three + four)

    gram = dot(raw_rows, raw_rows, 0, 0)
    gsend[0] = gram[:64]
    gsend[1] = gram[64:]
    gram_cross = send(gsend.at[1 - k], g1, other_core)

    raw_t = raw.T.astype(bf16)

    def image(half, part, store):
        columns = pl.ds(pl.multiple_of(half * (COLS // 2) + part * 256, 256), 256)
        block = dot(raw_t, mb[:, columns], 1, 0)
        store(part * 2, block[:, :128])
        store(part * 2 + 1, block[:, 128:])

    def store_far(at, block):
        rp[at] = block.astype(bf16)

    def store_near(at, block):
        rown[at] = block

    r_cross = []
    for chunk in (0, 1):
        for part in range(chunk * 4, chunk * 4 + 4):
            image(1 - k, part, store_far)
        piece = pl.ds(chunk * 8, 8)
        r_cross.append(send(rp.at[piece], r1.at[piece], other_core))

    for part in range(8):
        image(k, part, store_near)

    gram_cross.wait_recv()
    g2[a] = (gsend[k] + g1[...]).astype(bf16)
    gram_first = [send(g2.at[a], g2.at[a], first_axis(d)) for d in (2, 1, 3)]

    for copy in r_cross:
        copy.wait_recv()
    r_first = []
    for d in (2, 1, 3):
        to = lax.rem(a + d, 4)
        for j in range(4):
            s1[d - 1, j] = (rown[to * 4 + j] + r1[to * 4 + j].astype(f32)).astype(bf16)
        r_first.append(send(s1.at[d - 1], r2.at[d - 1], first_axis(d)))

    for copy in gram_first:
        copy.wait_recv()
    g3[b] = total_of(g2).astype(bf16)
    gram_second = [send(g3.at[b], g3.at[b], second_axis(d)) for d in (2, 1, 3)]

    for copy in r_first:
        copy.wait_recv()
    for j in range(4):
        s2[j] = (rown[a * 4 + j] + r1[a * 4 + j].astype(f32)) + (
            (r2[0, j].astype(f32) + r2[1, j].astype(f32)) + r2[2, j].astype(f32)
        )
    r_second = []
    for d in (2, 1, 3):
        s2b[d - 1] = s2[lax.rem(b + d, 4)].astype(bf16)
        r_second.append(send(s2b.at[d - 1], r3.at[d - 1], second_axis(d)))

    for copy in gram_second:
        copy.wait_recv()
    g4[h] = total_of(g3).astype(bf16)
    gram_third = send(g4.at[h], g4.at[h], other_half)

    for copy in r_second:
        copy.wait_recv()
    s3b[...] = (
        s2[b] + ((r3[0].astype(f32) + r3[1].astype(f32)) + r3[2].astype(f32))
    ).astype(bf16)
    r_third = send(s3b, r4, other_half)
    line_receive(1)
    line_send(2)
    line_send(3)

    gram_third.wait_recv()
    gfull[k] = g4[0].astype(f32) + g4[1].astype(f32)
    gram_last = send(gfull.at[k], gfull.at[k], other_core)
    gram_last.wait_recv()
    lower = inverse_lower(jnp.concatenate([gfull[0], gfull[1]], axis=0))

    r_third.wait_recv()
    image_sum = s3b[...].astype(f32) + r4[...].astype(f32)
    factor = dot(lower, image_sum, 1, 0, precise).astype(bf16)
    f_all[k, a, b, 0] = factor
    squared = jnp.square(factor.astype(f32))
    nb[b, c] = dot(jnp.ones((8, RANK), f32), squared, 1, 1, precise)

    square = nb.at[b, c]
    n_z = [send(square, square, along_z(d)) for d in (2, 1, 7)]
    z_copies = []
    for d, rows in ((2, pl.ds(0, 64)), (6, pl.ds(64, 64)), (1, pl.ds(0, 128)), (7, pl.ds(0, 128))):
        mine = f_all.at[k, a, b, 0, rows]
        z_copies.append(send(mine, f_all.at[k, a, b, (-d) % 4, rows], along_z(d)))

    up_a, down_a = first_axis(1), first_axis(3)
    up_b, down_b = second_axis(1), second_axis(3)
    a_below, a_above, a_far = lax.rem(a + 3, 4), lax.rem(a + 1, 4), lax.rem(a + 2, 4)
    b_below, b_above, b_far = lax.rem(b + 3, 4), lax.rem(b + 1, 4), lax.rem(b + 2, 4)

    def pass_on(at, islands, *devices):
        part = f_all.at[k, at[0], at[1], pl.ds(islands[0], islands[1] - islands[0])]
        return [send(part, part, device) for device in devices]

    early_b = pass_on((a, b), (0, 1), up_b, down_b)
    early_a = pass_on((a, b), (0, 1), up_a, down_a)
    basis = dot(raw_rows.astype(f32), lower, 1, 1, precise)[:OWN]
    p_all[c] = basis.astype(bf16)
    p_copies = [send(p_all.at[c], p_all.at[c], {"island": lax.rem(c + d, 4)}) for d in (1, 2, 3)]
    p_own[...] = (basis * (error_decay - 1.0)).astype(bf16)

    order = [lax.rem(m - c + 4, 4) for m in range(4)]

    def finish(half, at, groups=((0, 1), (2, 3))):
        for pieces in groups:
            every = [
                jnp.concatenate([f_all[half, i, at, order[m]] for m in range(4)], axis=0)
                for i in pieces
            ]
            mean = dot(p_scaled[...], jnp.concatenate(every, axis=1), 1, 0)
            own = [f_all[half, i, at, 0] for i in pieces]
            decay = dot(p_own[...], jnp.concatenate(own, axis=1), 1, 0)
            for n, i in enumerate(pieces):
                lanes = slice(n * 128, n * 128 + 128)
                columns = pl.ds(
                    pl.multiple_of(half * (COLS // 2) + i * 512 + at * 128, 128), 128
                )
                matrix = grads_v[:, columns].astype(f32) + buffer_v[:, columns].astype(f32)
                buffer_new[:, columns] = (matrix + decay[:, lanes]).astype(bf16)
                means[...] = mean[:, lanes]
                carried = jnp.concatenate(
                    [mom_all[m, :, columns].astype(f32) for m in range(4)], axis=0
                )
                part = mean[:, lanes]
                anchor_new[:, columns] = (
                    anchor_v[:, columns].astype(f32)
                    - outer_rate * (part + outer_beta * (outer_beta * carried + part))
                ).astype(bf16)
                rows = pl.ds(pl.multiple_of(c * QUARTER, 8), QUARTER)
                momentum_new[:, columns] = outer_beta * mom_v[:, columns] + means[rows, :]

    for copy in early_b:
        copy.wait_recv()
    early_b_on = pass_on((a, b_above), (0, 1), down_b)
    early_below = pass_on((a, b_below), (0, 1), up_a, down_a)
    early_above = pass_on((a, b_above), (0, 1), up_a, down_a)
    for copy in early_a:
        copy.wait_recv()
    early_a_on = pass_on((a_above, b), (0, 1), down_a)

    for copy in n_z:
        copy.wait_recv()
    n_second = [send(nb.at[b], nb.at[b], second_axis(d)) for d in (2, 1, 3)]
    for copy in z_copies:
        copy.wait_recv()
    up_copy, down_copy = pass_on((a, b), (1, 4), up_b, down_b)
    line_receive(2)
    line_send(4)
    for copy in n_second:
        copy.wait_recv()
    na[a] = (nb[0] + nb[1]) + (nb[2] + nb[3])
    n_first = [send(na.at[a], na.at[a], first_axis(d)) for d in (2, 1, 3)]
    own_up, own_down = pass_on((a, b), (1, 4), up_a, down_a)
    up_copy.wait_recv()
    b_on = pass_on((a, b_below), (2, 4), up_b)
    down_copy.wait_recv()
    b_on += pass_on((a, b_above), (1, 2), down_b)
    below_up, below_down = pass_on((a, b_below), (1, 4), up_a, down_a)
    above_up, above_down = pass_on((a, b_above), (1, 4), up_a, down_a)
    for copy in early_b_on + b_on:
        copy.wait_recv()
    far_up, far_down = pass_on((a, b_far), (0, 4), up_a, down_a)
    own_up.wait_recv()
    own_on = pass_on((a_below, b), (2, 4), up_a)
    own_down.wait_recv()
    own_on += pass_on((a_above, b), (1, 2), down_a)
    for copy in n_first:
        copy.wait_recv()
    nk[k] = (na[0] + na[1]) + (na[2] + na[3])
    n_cross = send(nk.at[k], nk.at[k], other_core)

    def forward_a(at, early, up, down):
        for copy in early:
            copy.wait_recv()
        up.wait_recv()
        on = pass_on((a_below, at), (2, 4), up_a)
        down.wait_recv()
        return on + pass_on((a_above, at), (0, 2), down_a)

    def cross(at, arriving):
        for copy in arriving:
            copy.wait_recv()
        part = f_all.at[k, :, at]
        return send(part, part, other_core)

    below_on = forward_a(b_below, early_below, below_up, below_down)
    above_on = forward_a(b_above, early_above, above_up, above_down)
    far_on = forward_a(b_far, [], far_up, far_down)
    far_cross = []
    for i in (a, a_below, a_above, a_far):
        part = f_all.at[k, i, b_far]
        far_cross.append(copy_to(part, part, other_core))
    for copy in far_cross[:3]:
        copy.start()
    n_cross.wait_recv()
    for copy in p_copies:
        copy.wait_recv()
    rate = math.sqrt(ROWS * COLS / RANK) / 4.0
    for island in range(4):
        total = (nk[0, island] + nk[1, island])[:1]
        scale = rate * lax.rsqrt(total + epsilon)
        p_scaled[:, island * RANK : (island + 1) * RANK] = (
            p_all[island].astype(f32) * scale
        ).astype(bf16)
    loads[3].wait()
    crossing = [cross(b, early_a_on + own_on)]
    line_receive(3)
    line_receive(4)
    finish(k, b)
    crossing.append(cross(b_below, below_on))
    crossing.append(cross(b_above, above_on))
    finish(k, b_below)
    finish(k, b_above)
    crossing[0].wait_recv()
    finish(1 - k, a)
    for copy in far_on:
        copy.wait_recv()
    far_cross[3].start()
    for copy, at in zip(crossing[1:3], (a_below, a_above)):
        copy.wait_recv()
        finish(1 - k, at)
    finish(k, b_far)
    for copy in far_cross[:3]:
        copy.wait_recv()
    finish(1 - k, a_far, ((b_below, b_above),))
    far_cross[3].wait_recv()
    finish(1 - k, a_far, ((b, b_far),))
    started.extend(far_cross)
    for copy in started:
        copy.wait_send()


def exchange(grads, buffer, q_old, anchor, momentum):
    vmem = pltpu.VMEM
    whole = pl.BlockSpec(memory_space=pltpu.VMEM)
    anywhere = pl.BlockSpec(memory_space=pltpu.HBM)
    block = (128, 128)
    return pl.pallas_call(
        exchange_kernel,
        out_shape=(
            vmem((OWN, COLS), bf16),
            vmem((OWN, COLS), bf16),
            vmem((QUARTER, COLS), f32),
        ),
        in_specs=[anywhere] * 5,
        out_specs=(whole, whole, whole),
        scratch_shapes=[
            vmem((2, 4, 4, 4, *block), bf16),
            vmem((OWN, 4 * RANK), bf16),
            vmem((OWN, RANK), bf16),
            vmem((4, QUARTER, COLS), bf16),
            vmem((OWN, COLS), bf16),
            vmem((OWN, 128), f32),
            vmem((4, 4, 8, 128), f32),
            vmem((4, 4, 8, 128), f32),
            vmem((2, 4, 8, 128), f32),
            vmem((64, RANK), f32),
            vmem((OWN, COLS), bf16),
            vmem((OWN, COLS), bf16),
            vmem((QUARTER, COLS), f32),
            vmem((PADDED, COLS), bf16),
            vmem((2, 2, PADDED, COLS // 4), bf16),
            vmem((2, 2, 4, 4, 64, RANK), bf16),
            vmem((PADDED, RANK), bf16),
            vmem((2, 64, 128), f32),
            vmem((64, 128), f32),
            vmem((4, 64, 128), bf16),
            vmem((4, 64, 128), bf16),
            vmem((2, 64, 128), bf16),
            vmem((2, 64, 128), f32),
            vmem((16, *block), bf16),
            vmem((16, *block), f32),
            vmem((16, *block), bf16),
            vmem((3, 4, *block), bf16),
            vmem((3, 4, *block), bf16),
            vmem((4, *block), f32),
            vmem((3, *block), bf16),
            vmem((3, *block), bf16),
            vmem(block, bf16),
            vmem(block, bf16),
            vmem((4, OWN, RANK), bf16),
            pltpu.SemaphoreType.DMA((5,)),
            pltpu.SemaphoreType.DMA((160,)),
            pltpu.SemaphoreType.DMA((160,)),
        ],
        compiler_params=pltpu.CompilerParams(
            collective_id=0, has_side_effects=True, vmem_limit_bytes=36 * 1024 * 1024
        ),
        name="exchange",
    )(*(pltpu.with_memory_space_constraint(v, pltpu.HBM) for v in (grads, buffer, q_old, anchor, momentum)))


def store_kernel(anchor_v, buffer_v, momentum_v, anchor_new, buffer_new, momentum_new, sems):
    copies = []
    for source, target, parts in (
        (anchor_v, anchor_new, 7),
        (buffer_v, buffer_new, 7),
        (momentum_v, momentum_new, 7),
    ):
        height = source.shape[0] // parts
        for part in range(parts):
            rows = pl.ds(part * height, height)
            copy = pltpu.make_async_copy(source.at[rows], target.at[rows], sems.at[len(copies)])
            copy.start()
            copies.append(copy)
    for copy in copies:
        copy.wait()


def store(anchor_new, buffer_new, momentum_new):
    return pl.pallas_call(
        store_kernel,
        out_shape=(
            jax.ShapeDtypeStruct((OWN, COLS), bf16),
            jax.ShapeDtypeStruct((OWN, COLS), bf16),
            jax.ShapeDtypeStruct((QUARTER, COLS), f32),
        ),
        in_specs=[pl.BlockSpec(memory_space=pltpu.VMEM)] * 3,
        out_specs=[pl.BlockSpec(memory_space=pltpu.HBM)] * 3,
        scratch_shapes=[pltpu.SemaphoreType.DMA((21,))],
        compiler_params=pltpu.CompilerParams(vmem_limit_bytes=1024 * 1024),
        name="store",
    )(anchor_new, buffer_new, momentum_new)


def body(grads, buffer, q_old, anchor, momentum):
    anchor_new, buffer_new, momentum_new = store(
        *exchange(grads[0, 0], buffer[0], q_old[0], anchor, momentum)
    )
    return (anchor_new, buffer_new[None], momentum_new)


def solution(mesh):
    split = Mesh(
        mesh.devices.reshape(mesh.shape["island"], 2, 4, 4, 2),
        ("island", "fsdp_0", "fsdp_1", "fsdp_2", "fsdp_3"),
    )
    return jax.shard_map(
        body,
        mesh=split,
        in_specs=(
            P("island", None, FSDP, None),
            P("island", FSDP, None),
            P("island", FSDP, None),
            P(FSDP, None),
            P(FSDP_ISLAND, None),
        ),
        out_specs=(P(FSDP, None), P("island", FSDP, None), P(FSDP_ISLAND, None)),
        check_vma=False,
    )
```

```python
import math

import jax
import jax.numpy as jnp
from jax import lax
from jax.experimental import pallas as pl
from jax.experimental.pallas import tpu as pltpu
from jax.sharding import Mesh
from jax.sharding import PartitionSpec as P

ROWS = 14336
COLS = 4096
RANK = 128
FSDP = ("fsdp_0", "fsdp_1", "fsdp_2", "fsdp_3")
FSDP_ISLAND = ("fsdp_0", "fsdp_1", "fsdp_2", "fsdp_3", "island")
OWN = 224
PADDED = 256
QUARTER = 56
SENDS, RECEIVES = 64, 115
MESH = pl.DeviceIdType.MESH

precise = lax.Precision.HIGHEST
error_decay = 0.95
outer_beta = 0.9
outer_rate = 0.7
epsilon = 1e-06
f32 = jnp.float32
bf16 = jnp.bfloat16


def dot(left, right, left_dim, right_dim, precision=None):
    return lax.dot_general(
        left,
        right,
        (((left_dim,), (right_dim,)), ((), ())),
        precision=precision,
        preferred_element_type=f32,
    )


def inverse_lower(gram, width=8):
    n = gram.shape[0]
    rest = gram
    side = (
        lax.broadcasted_iota(jnp.int32, (n, n), 0) == lax.broadcasted_iota(jnp.int32, (n, n), 1)
    ).astype(f32)
    done = []
    for first in range(0, n, 8):
        rows = lax.broadcasted_iota(jnp.int32, rest.shape, 0)
        scale = jnp.ones((8, n), f32)
        head = lax.broadcasted_iota(jnp.int32, (8, n), 0)
        for at in range(0, 8, width):
            columns = [
                jnp.broadcast_to(rest[:, first + at + i : first + at + i + 1], rest.shape)
                for i in range(width)
            ]
            for i in range(width):
                row = at + i
                pivot = columns[i][row : row + 1, :]
                times = jnp.where(rows > row, columns[i] * (1.0 / pivot), 0.0)
                scale = jnp.where(head == row, pivot, scale)
                for j in range(i + 1, width):
                    columns[j] = columns[j] - times * columns[j][row : row + 1, :]
                rest = rest - times * rest[row : row + 1, :]
                side = side - times * side[row : row + 1, :]
        done.append(side[:8] * lax.rsqrt(scale))
        rest, side = rest[8:], side[8:]
    return jnp.concatenate(done, axis=0)


def first_column(half, i, at):
    return pl.multiple_of(half * (COLS // 2) + i * 512 + at * 128, 128)


def finish_columns(c, half, at, held, outs, means, place=None):
    f_all, p_scaled, p_own, mom_all, grads_v, buffer_v, anchor_v, mom_v = held
    anchor_new, buffer_new, momentum_new = outs
    order = [lax.rem(m - c + 4, 4) for m in range(4)]
    for pieces in ((0, 1), (2, 3)):
        every = [
            jnp.concatenate([f_all[half, i, at, order[m]] for m in range(4)], axis=0)
            for i in pieces
        ]
        mean = dot(p_scaled[...], jnp.concatenate(every, axis=1), 1, 0)
        own = [f_all[half, i, at, 0] for i in pieces]
        decay = dot(p_own[...], jnp.concatenate(own, axis=1), 1, 0)
        for n, i in enumerate(pieces):
            lanes = slice(n * 128, n * 128 + 128)
            columns = pl.ds(first_column(half, i, at), 128)
            target = columns if place is None else pl.ds((place + i) * 128, 128)
            matrix = grads_v[:, columns].astype(f32) + buffer_v[:, columns].astype(f32)
            buffer_new[:, target] = (matrix + decay[:, lanes]).astype(bf16)
            part = mean[:, lanes]
            means[...] = part
            carried = jnp.concatenate(
                [mom_all[m, :, columns].astype(f32) for m in range(4)], axis=0
            )
            anchor_new[:, target] = (
                anchor_v[:, columns].astype(f32)
                - outer_rate * (part + outer_beta * (outer_beta * carried + part))
            ).astype(bf16)
            rows = pl.ds(pl.multiple_of(c * QUARTER, 8), QUARTER)
            momentum_new[:, target] = outer_beta * mom_v[:, columns] + means[rows, :]


def exchange_kernel(
    grads,
    buffer,
    q_old,
    anchor,
    momentum,
    anchor_new,
    buffer_new,
    momentum_new,
    f_all,
    p_scaled,
    p_own,
    mom_all,
    grads_v,
    buffer_v,
    anchor_v,
    mom_v,
    means,
    nb,
    na,
    nk,
    q_v,
    mb,
    mp,
    qa,
    raw_b,
    gsend,
    g1,
    g2,
    g3,
    g4,
    gfull,
    rp,
    rown,
    r1,
    s1,
    r2,
    s2,
    s2b,
    r3,
    s3b,
    r4,
    p_all,
    load_sem,
    send_sem,
    recv_sem,
):
    c = lax.axis_index("island")
    h = lax.axis_index("fsdp_0")
    x = lax.axis_index("fsdp_1")
    y = lax.axis_index("fsdp_2")
    k = lax.axis_index("fsdp_3")
    z = h * 4 + c
    a = x * (1 - k) + y * k
    b = y * (1 - k) + x * k

    def first_axis(d):
        return {"fsdp_1": lax.rem(x + d * (1 - k), 4), "fsdp_2": lax.rem(y + d * k, 4)}

    def second_axis(d):
        return {"fsdp_1": lax.rem(x + d * k, 4), "fsdp_2": lax.rem(y + d * (1 - k), 4)}

    def along_z(d):
        to = lax.rem(z + d, 8)
        return {"fsdp_0": to // 4, "island": lax.rem(to, 4)}

    other_core = {"fsdp_3": 1 - k}
    other_half = {"fsdp_0": 1 - h}

    peers = [other_core, other_half]
    for d in (1, 2, 3):
        peers.append({"fsdp_1": lax.rem(x + d, 4)})
        peers.append({"fsdp_2": lax.rem(y + d, 4)})
        peers.append({"island": lax.rem(c + d, 4)})
    for d in (1, 2, 6, 7):
        peers.append(along_z(d))

    receives = iter(range(RECEIVES))
    free = list(range(SENDS))
    started = []

    def copy_to(src, dst, device, at=None):
        return pltpu.make_async_remote_copy(
            src_ref=src,
            dst_ref=dst,
            send_sem=send_sem.at[free.pop() if at is None else at],
            recv_sem=recv_sem.at[next(receives)],
            device_id=device,
            device_id_type=MESH,
        )

    def send(src, dst, device):
        at = free.pop()
        copy = copy_to(src, dst, device, at)
        copy.start()
        started.append((at, copy))
        return copy

    def sends_done():
        for at, copy in started:
            copy.wait_send()
            free.append(at)
        started.clear()

    barrier = pltpu.get_barrier_semaphore()
    for peer in peers:
        pl.semaphore_signal(barrier, inc=1, device_id=peer, device_id_type=MESH)

    loads = [
        pltpu.make_async_copy(momentum, mom_v, load_sem.at[0]),
        pltpu.make_async_copy(grads, grads_v, load_sem.at[1]),
        pltpu.make_async_copy(buffer, buffer_v, load_sem.at[2]),
        pltpu.make_async_copy(anchor, anchor_v, load_sem.at[3]),
        pltpu.make_async_copy(q_old, q_v, load_sem.at[4]),
    ]
    for at in (4, 0, 1, 2, 3):
        loads[at].start()
    loads[4].wait()
    qa[h, k, a, b] = q_v[...].astype(bf16)
    pl.semaphore_wait(barrier, len(peers))

    def along_second(part):
        return [send(part, part, second_axis(d)) for d in (2, 1, 3)]

    def first_sends(part):
        return {d: send(part, part, first_axis(d)) for d in (2, 1, 3)}

    own_piece = qa.at[h, k, a, b]
    far_piece = qa.at[1 - h, k, a, b]
    q_far = send(own_piece, own_piece, other_half)
    q_first = first_sends(own_piece)
    on_near = along_second(own_piece)

    line = []
    for step, first, rows in ((1, 0, 56), (2, 0, 40), (2, 40, 16), (3, 0, 16), (3, 16, 40)):
        up_ok = jnp.logical_and(c < 3, c >= step - 1)
        down_ok = jnp.logical_and(c > 0, c + step - 1 <= 3)
        up_part = mom_all.at[lax.rem(c - (step - 1) + 4, 4), pl.ds(first, rows)]
        down_part = mom_all.at[lax.rem(c + (step - 1), 4), pl.ds(first, rows)]
        up = copy_to(up_part, up_part, {"island": lax.rem(c + 1, 4)})
        down = copy_to(down_part, down_part, {"island": lax.rem(c + 3, 4)})
        line.append((up_ok, up, c - step >= 0, down_ok, down, c + step <= 3))

    def line_send(hop):
        up_ok, up, _, down_ok, down, _ = line[hop]

        @pl.when(up_ok)
        def _():
            up.start()

        @pl.when(down_ok)
        def _():
            down.start()

    def line_receive(hop):
        up_ok, up, from_below, down_ok, down, from_above = line[hop]

        @pl.when(from_below)
        def _():
            up.wait_recv()

        @pl.when(from_above)
        def _():
            down.wait_recv()

        @pl.when(up_ok)
        def _():
            up.wait_send()

        @pl.when(down_ok)
        def _():
            down.wait_send()

    loads[0].wait()
    mom_all[c] = mom_v[...].astype(bf16)
    line_send(0)

    loads[1].wait()
    loads[2].wait()

    low_lanes = lax.broadcasted_iota(jnp.int32, (16, 128), 1) < 64

    @pl.loop(0, OWN // 16)
    def _(i):
        at = pl.ds(pl.multiple_of(i * 16, 16), 16)
        matrix = grads_v[at, :].astype(f32) + buffer_v[at, :].astype(f32)
        mb[at, :] = matrix.astype(bf16)

        def block(half, row, column):
            first = (half * 16 + row * 4 + column) * 128
            return matrix[:, first : first + 128]

        for half in (0, 1):
            for outer in range(4):
                for pair in (0, 1):
                    lanes = slice((outer * 2 + pair) * 128, (outer * 2 + pair + 1) * 128)
                    one, two = block(half, outer, pair * 2), block(half, outer, pair * 2 + 1)
                    mp[half, 0, at, lanes] = jnp.where(
                        low_lanes, one, pltpu.roll(two, 64, 1)
                    ).astype(bf16)
                    one, two = block(half, pair * 2, outer), block(half, pair * 2 + 1, outer)
                    mp[half, 1, at, lanes] = jnp.where(
                        low_lanes, pltpu.roll(one, 64, 1), two
                    ).astype(bf16)

    mb[OWN:, :] = jnp.zeros((PADDED - OWN, COLS), bf16)
    for half in (0, 1):
        for core in (0, 1):
            mp[half, core, OWN:, :] = jnp.zeros((PADDED - OWN, COLS // 4), bf16)

    def arrived(at, copies):
        on = []
        for d in (1, 3, 2):
            copies[d].wait_recv()
            on += along_second(qa.at[at, k, lax.rem(a + 4 - d, 4), b])
        return on

    on_near += arrived(h, q_first)
    q_far.wait_recv()
    q_first = first_sends(far_piece)
    on_far = along_second(far_piece)
    on_far += arrived(1 - h, q_first)
    q_second = [(h, on_near), (1 - h, on_far)]
    q_cross = []
    for at, copies in q_second:
        for copy in copies:
            copy.wait_recv()
        half = qa.at[at, k]
        q_cross.append((at, send(half, half, other_core)))

    line_receive(0)
    line_send(1)
    raw = jnp.zeros((PADDED, RANK), f32)
    for at, copy in q_cross:
        raw = raw + dot(mp[at, k], qa[at, k].reshape(COLS // 4, RANK), 1, 0)
        copy.wait_recv()
        raw = raw + dot(mp[at, 1 - k], qa[at, 1 - k].reshape(COLS // 4, RANK), 1, 0)
    raw_b[...] = raw.astype(bf16)
    raw_rows = raw_b[...]

    def total_of(parts):
        one, two, three, four = (parts[i].astype(f32) for i in range(4))
        return (one + two) + (three + four)

    sends_done()
    gram = dot(raw_rows, raw_rows, 0, 0)
    gsend[0] = gram[:64]
    gsend[1] = gram[64:]
    gram_cross = send(gsend.at[1 - k], g1, other_core)

    raw_t = raw.T.astype(bf16)

    def image(half, part, store):
        columns = pl.ds(pl.multiple_of(half * (COLS // 2) + part * 256, 256), 256)
        block = dot(raw_t, mb[:, columns], 1, 0)
        store(part * 2, block[:, :128])
        store(part * 2 + 1, block[:, 128:])

    def store_far(at, block):
        rp[at] = block.astype(bf16)

    def store_near(at, block):
        rown[at] = block

    r_cross = []
    for chunk in (0, 1):
        for part in range(chunk * 4, chunk * 4 + 4):
            image(1 - k, part, store_far)
        piece = pl.ds(chunk * 8, 8)
        r_cross.append(send(rp.at[piece], r1.at[piece], other_core))

    for part in range(8):
        image(k, part, store_near)

    gram_cross.wait_recv()
    g2[a] = (gsend[k] + g1[...]).astype(bf16)
    gram_first = [send(g2.at[a], g2.at[a], first_axis(d)) for d in (2, 1, 3)]

    for copy in r_cross:
        copy.wait_recv()
    r_first = []
    for d in (2, 1, 3):
        to = lax.rem(a + d, 4)
        for j in range(4):
            s1[d - 1, j] = (rown[to * 4 + j] + r1[to * 4 + j].astype(f32)).astype(bf16)
        r_first.append(send(s1.at[d - 1], r2.at[d - 1], first_axis(d)))

    for copy in gram_first:
        copy.wait_recv()
    g3[b] = total_of(g2).astype(bf16)
    gram_second = [send(g3.at[b], g3.at[b], second_axis(d)) for d in (2, 1, 3)]

    for copy in r_first:
        copy.wait_recv()
    for j in range(4):
        s2[j] = (rown[a * 4 + j] + r1[a * 4 + j].astype(f32)) + (
            (r2[0, j].astype(f32) + r2[1, j].astype(f32)) + r2[2, j].astype(f32)
        )
    r_second = []
    for d in (2, 1, 3):
        s2b[d - 1] = s2[lax.rem(b + d, 4)].astype(bf16)
        r_second.append(send(s2b.at[d - 1], r3.at[d - 1], second_axis(d)))

    for copy in gram_second:
        copy.wait_recv()
    g4[h] = total_of(g3).astype(bf16)
    gram_third = send(g4.at[h], g4.at[h], other_half)

    for copy in r_second:
        copy.wait_recv()
    s3b[...] = (
        s2[b] + ((r3[0].astype(f32) + r3[1].astype(f32)) + r3[2].astype(f32))
    ).astype(bf16)
    r_third = send(s3b, r4, other_half)
    line_receive(1)
    line_send(2)
    line_send(3)

    gram_third.wait_recv()
    gfull[k] = g4[0].astype(f32) + g4[1].astype(f32)
    gram_last = send(gfull.at[k], gfull.at[k], other_core)
    gram_last.wait_recv()
    lower = inverse_lower(jnp.concatenate([gfull[0], gfull[1]], axis=0))

    r_third.wait_recv()
    image_sum = s3b[...].astype(f32) + r4[...].astype(f32)
    factor = dot(lower, image_sum, 1, 0, precise).astype(bf16)
    f_all[k, a, b, 0] = factor
    squared = jnp.square(factor.astype(f32))
    nb[b, c] = dot(jnp.ones((8, RANK), f32), squared, 1, 1, precise)

    sends_done()
    square = nb.at[b, c]
    n_z = [send(square, square, along_z(d)) for d in (2, 1, 7)]
    z_copies = []
    for d, rows in ((2, pl.ds(0, 64)), (6, pl.ds(64, 64)), (1, pl.ds(0, 128)), (7, pl.ds(0, 128))):
        mine = f_all.at[k, a, b, 0, rows]
        z_copies.append(send(mine, f_all.at[k, a, b, (-d) % 4, rows], along_z(d)))

    up_a, down_a = first_axis(1), first_axis(3)
    up_b, down_b = second_axis(1), second_axis(3)
    a_below, a_above, a_far = lax.rem(a + 3, 4), lax.rem(a + 1, 4), lax.rem(a + 2, 4)
    b_below, b_above, b_far = lax.rem(b + 3, 4), lax.rem(b + 1, 4), lax.rem(b + 2, 4)

    def pass_on(at, islands, *devices):
        part = f_all.at[k, at[0], at[1], pl.ds(islands[0], islands[1] - islands[0])]
        return [send(part, part, device) for device in devices]

    early_b = pass_on((a, b), (0, 1), up_b, down_b)
    early_a = pass_on((a, b), (0, 1), up_a, down_a)
    basis = dot(raw_rows.astype(f32), lower, 1, 1, precise)[:OWN]
    p_all[c] = basis.astype(bf16)
    p_own[...] = (basis * (error_decay - 1.0)).astype(bf16)

    held = (f_all, p_scaled, p_own, mom_all, grads_v, buffer_v, anchor_v, mom_v)
    outs = (anchor_new, buffer_new, momentum_new)

    def finish(half, at):
        finish_columns(c, half, at, held, outs, means)

    for copy in early_b:
        copy.wait_recv()
    early_b_on = pass_on((a, b_above), (0, 1), down_b)
    early_below = pass_on((a, b_below), (0, 1), up_a, down_a)
    early_above = pass_on((a, b_above), (0, 1), up_a, down_a)
    for copy in early_a:
        copy.wait_recv()
    early_a_on = pass_on((a_above, b), (0, 1), down_a)

    for copy in n_z:
        copy.wait_recv()
    n_second = [send(nb.at[b], nb.at[b], second_axis(d)) for d in (2, 1, 3)]
    for copy in z_copies:
        copy.wait_recv()
    up_copy, down_copy = pass_on((a, b), (1, 4), up_b, down_b)
    p_copies = [send(p_all.at[c], p_all.at[c], {"island": lax.rem(c + d, 4)}) for d in (1, 2, 3)]
    for copy in n_second:
        copy.wait_recv()
    na[a] = (nb[0] + nb[1]) + (nb[2] + nb[3])
    n_first = [send(na.at[a], na.at[a], first_axis(d)) for d in (2, 1, 3)]
    own_up, own_down = pass_on((a, b), (1, 4), up_a, down_a)
    up_copy.wait_recv()
    b_on = pass_on((a, b_below), (2, 4), up_b)
    down_copy.wait_recv()
    b_on += pass_on((a, b_above), (1, 2), down_b)
    below_up, below_down = pass_on((a, b_below), (1, 4), up_a, down_a)
    above_up, above_down = pass_on((a, b_above), (1, 4), up_a, down_a)
    line_receive(2)
    line_send(4)
    for copy in early_b_on + b_on:
        copy.wait_recv()
    far_up, far_down = pass_on((a, b_far), (0, 4), up_a, down_a)
    own_up.wait_recv()
    own_on = pass_on((a_below, b), (2, 4), up_a)
    own_down.wait_recv()
    own_on += pass_on((a_above, b), (1, 2), down_a)
    for copy in n_first:
        copy.wait_recv()
    nk[k] = (na[0] + na[1]) + (na[2] + na[3])
    n_cross = send(nk.at[k], nk.at[k], other_core)

    def forward_a(at, early, up, down):
        for copy in early:
            copy.wait_recv()
        up.wait_recv()
        on = pass_on((a_below, at), (2, 4), up_a)
        down.wait_recv()
        return on + pass_on((a_above, at), (0, 2), down_a)

    def cross(at, arriving):
        for copy in arriving:
            copy.wait_recv()
        part = f_all.at[k, :, at]
        return send(part, part, other_core)

    below_on = forward_a(b_below, early_below, below_up, below_down)
    above_on = forward_a(b_above, early_above, above_up, above_down)
    far_on = forward_a(b_far, [], far_up, far_down)
    far_cross = []
    for i in (a, a_below, a_above, a_far):
        part = f_all.at[k, i, b_far]
        far_cross.append(copy_to(part, part, other_core))
    for copy in far_cross[:3]:
        copy.start()
    n_cross.wait_recv()
    for copy in p_copies:
        copy.wait_recv()
    rate = math.sqrt(ROWS * COLS / RANK) / 4.0
    for island in range(4):
        total = (nk[0, island] + nk[1, island])[:1]
        scale = rate * lax.rsqrt(total + epsilon)
        p_scaled[:, island * RANK : (island + 1) * RANK] = (
            p_all[island].astype(f32) * scale
        ).astype(bf16)
    loads[3].wait()
    crossing = [cross(b, early_a_on + own_on)]
    line_receive(3)
    line_receive(4)
    finish(k, b)
    crossing.append(cross(b_below, below_on))
    crossing.append(cross(b_above, above_on))
    finish(k, b_below)
    finish(k, b_above)
    crossing[0].wait_recv()
    finish(1 - k, a)
    for copy in far_on:
        copy.wait_recv()
    far_cross[3].start()
    crossing[1].wait_recv()
    finish(1 - k, a_below)
    finish(k, b_far)
    for copy in crossing[2:] + far_cross:
        copy.wait_recv()
    sends_done()
    for copy in far_cross:
        copy.wait_send()


def exchange(grads, buffer, q_old, anchor, momentum):
    vmem = pltpu.VMEM
    whole = pl.BlockSpec(memory_space=pltpu.VMEM)
    anywhere = pl.BlockSpec(memory_space=pltpu.HBM)
    block = (128, 128)
    return pl.pallas_call(
        exchange_kernel,
        out_shape=(
            vmem((OWN, COLS), bf16),
            vmem((OWN, COLS), bf16),
            vmem((QUARTER, COLS), f32),
            vmem((2, 4, 4, 4, *block), bf16),
            vmem((OWN, 4 * RANK), bf16),
            vmem((OWN, RANK), bf16),
            vmem((4, QUARTER, COLS), bf16),
            vmem((OWN, COLS), bf16),
            vmem((OWN, COLS), bf16),
            vmem((OWN, COLS), bf16),
            vmem((QUARTER, COLS), f32),
        ),
        in_specs=[anywhere] * 5,
        out_specs=(whole,) * 11,
        scratch_shapes=[
            vmem((OWN, 128), f32),
            vmem((4, 4, 8, 128), f32),
            vmem((4, 4, 8, 128), f32),
            vmem((2, 4, 8, 128), f32),
            vmem((64, RANK), f32),
            vmem((PADDED, COLS), bf16),
            vmem((2, 2, PADDED, COLS // 4), bf16),
            vmem((2, 2, 4, 4, 64, RANK), bf16),
            vmem((PADDED, RANK), bf16),
            vmem((2, 64, 128), f32),
            vmem((64, 128), f32),
            vmem((4, 64, 128), bf16),
            vmem((4, 64, 128), bf16),
            vmem((2, 64, 128), bf16),
            vmem((2, 64, 128), f32),
            vmem((16, *block), bf16),
            vmem((16, *block), f32),
            vmem((16, *block), bf16),
            vmem((3, 4, *block), bf16),
            vmem((3, 4, *block), bf16),
            vmem((4, *block), f32),
            vmem((3, *block), bf16),
            vmem((3, *block), bf16),
            vmem(block, bf16),
            vmem(block, bf16),
            vmem((4, OWN, RANK), bf16),
            pltpu.SemaphoreType.DMA((5,)),
            pltpu.SemaphoreType.DMA((SENDS,)),
            pltpu.SemaphoreType.DMA((RECEIVES,)),
        ],
        compiler_params=pltpu.CompilerParams(
            collective_id=0, has_side_effects=True, vmem_limit_bytes=32 * 1024 * 1024
        ),
        name="exchange",
    )(*(pltpu.with_memory_space_constraint(v, pltpu.HBM) for v in (grads, buffer, q_old, anchor, momentum)))


def update_kernel(*refs):
    done, held, outs, parts = refs[:3], refs[3:11], refs[11:14], refs[14:17]
    means, *sems = refs[17:]
    c = lax.axis_index("island")
    x = lax.axis_index("fsdp_1")
    y = lax.axis_index("fsdp_2")
    k = lax.axis_index("fsdp_3")
    a = x * (1 - k) + y * k

    def copy_columns(sources, first, to, width):
        for source, out, sem in zip(sources, outs, sems):
            copy = pltpu.make_async_copy(
                source.at[:, pl.ds(first, width)],
                out.at[:, pl.ds(to, width)],
                sem,
            )
            copy.start()

    for quarter in range(2):
        first = pl.multiple_of(k * (COLS // 2) + quarter * 1024, 1024)
        copy_columns(done, first, first, 1024)
    for at in (a, lax.rem(a + 3, 4)):
        for i in range(4):
            first = first_column(1 - k, i, at)
            copy_columns(done, first, first, 128)
    for n, at in enumerate((lax.rem(a + 1, 4), lax.rem(a + 2, 4))):
        finish_columns(c, 1 - k, at, held, parts, means, place=n * 4)
        for i in range(4):
            copy_columns(parts, (n * 4 + i) * 128, first_column(1 - k, i, at), 128)
    for source, out, sem in zip(done, outs, sems):
        pltpu.make_async_copy(source, out, sem).wait()


def update(*arrays):
    return pl.pallas_call(
        update_kernel,
        out_shape=(
            jax.ShapeDtypeStruct((OWN, COLS), bf16),
            jax.ShapeDtypeStruct((OWN, COLS), bf16),
            jax.ShapeDtypeStruct((QUARTER, COLS), f32),
        ),
        in_specs=[pl.BlockSpec(memory_space=pltpu.VMEM)] * 11,
        out_specs=[pl.BlockSpec(memory_space=pltpu.HBM)] * 3,
        scratch_shapes=[
            pltpu.VMEM((OWN, 1024), bf16),
            pltpu.VMEM((OWN, 1024), bf16),
            pltpu.VMEM((QUARTER, 1024), f32),
            pltpu.VMEM((OWN, 128), f32),
            pltpu.SemaphoreType.DMA,
            pltpu.SemaphoreType.DMA,
            pltpu.SemaphoreType.DMA,
        ],
        compiler_params=pltpu.CompilerParams(vmem_limit_bytes=8 * 1024 * 1024),
        name="update",
    )(*arrays)


def body(grads, buffer, q_old, anchor, momentum):
    anchor_new, buffer_new, momentum_new = update(
        *exchange(grads[0, 0], buffer[0], q_old[0], anchor, momentum)
    )
    return (anchor_new, buffer_new[None], momentum_new)


def solution(mesh):
    split = Mesh(
        mesh.devices.reshape(mesh.shape["island"], 2, 4, 4, 2),
        ("island", "fsdp_0", "fsdp_1", "fsdp_2", "fsdp_3"),
    )
    return jax.shard_map(
        body,
        mesh=split,
        in_specs=(
            P("island", None, FSDP, None),
            P("island", FSDP, None),
            P("island", FSDP, None),
            P(FSDP, None),
            P(FSDP_ISLAND, None),
        ),
        out_specs=(P(FSDP, None), P("island", FSDP, None), P(FSDP_ISLAND, None)),
        check_vma=False,
    )
```

```python
import math

import jax
import jax.numpy as jnp
from jax import lax
from jax.experimental import pallas as pl
from jax.experimental.pallas import tpu as pltpu
from jax.sharding import Mesh
from jax.sharding import PartitionSpec as P

ROWS = 14336
COLS = 4096
RANK = 128
FSDP = ("fsdp_0", "fsdp_1", "fsdp_2", "fsdp_3")
FSDP_ISLAND = ("fsdp_0", "fsdp_1", "fsdp_2", "fsdp_3", "island")
OWN = 224
PADDED = 256
QUARTER = 56
SENDS, RECEIVES = 64, 93
MESH = pl.DeviceIdType.MESH

precise = lax.Precision.HIGHEST
error_decay = 0.95
outer_beta = 0.9
outer_rate = 0.7
epsilon = 1e-06
f32 = jnp.float32
bf16 = jnp.bfloat16


def dot(left, right, left_dim, right_dim, precision=None):
    return lax.dot_general(
        left,
        right,
        (((left_dim,), (right_dim,)), ((), ())),
        precision=precision,
        preferred_element_type=f32,
    )


def inverse_lower(gram, width=8):
    n = gram.shape[0]
    rest = gram
    side = (
        lax.broadcasted_iota(jnp.int32, (n, n), 0) == lax.broadcasted_iota(jnp.int32, (n, n), 1)
    ).astype(f32)
    done = []
    for first in range(0, n, 8):
        rows = lax.broadcasted_iota(jnp.int32, rest.shape, 0)
        scale = jnp.ones((8, n), f32)
        head = lax.broadcasted_iota(jnp.int32, (8, n), 0)
        for at in range(0, 8, width):
            columns = [
                jnp.broadcast_to(rest[:, first + at + i : first + at + i + 1], rest.shape)
                for i in range(width)
            ]
            for i in range(width):
                row = at + i
                pivot = columns[i][row : row + 1, :]
                times = jnp.where(rows > row, columns[i] * (1.0 / pivot), 0.0)
                scale = jnp.where(head == row, pivot, scale)
                for j in range(i + 1, width):
                    columns[j] = columns[j] - times * columns[j][row : row + 1, :]
                rest = rest - times * rest[row : row + 1, :]
                side = side - times * side[row : row + 1, :]
        done.append(side[:8] * lax.rsqrt(scale))
        rest, side = rest[8:], side[8:]
    return jnp.concatenate(done, axis=0)


def first_column(half, i, at):
    return pl.multiple_of(half * (COLS // 2) + i * 512 + at * 128, 128)


def finish_columns(c, half, at, held, outs, means, place=None):
    f_all, p_scaled, p_own, mom_all, grads_v, buffer_v, anchor_v, mom_v = held
    anchor_new, buffer_new, momentum_new = outs
    order = [lax.rem(m - c + 4, 4) for m in range(4)]
    for pieces in ((0, 1), (2, 3)):
        every = [
            jnp.concatenate([f_all[half, i, at, order[m]] for m in range(4)], axis=0)
            for i in pieces
        ]
        mean = dot(p_scaled[...], jnp.concatenate(every, axis=1), 1, 0)
        own = [f_all[half, i, at, 0] for i in pieces]
        decay = dot(p_own[...], jnp.concatenate(own, axis=1), 1, 0)
        for n, i in enumerate(pieces):
            lanes = slice(n * 128, n * 128 + 128)
            columns = pl.ds(first_column(half, i, at), 128)
            target = columns if place is None else pl.ds((place + i) * 128, 128)
            matrix = grads_v[:, columns].astype(f32) + buffer_v[:, columns].astype(f32)
            buffer_new[:, target] = (matrix + decay[:, lanes]).astype(bf16)
            part = mean[:, lanes]
            means[...] = part
            carried = jnp.concatenate(
                [mom_all[m, :, columns].astype(f32) for m in range(4)], axis=0
            )
            anchor_new[:, target] = (
                anchor_v[:, columns].astype(f32)
                - outer_rate * (part + outer_beta * (outer_beta * carried + part))
            ).astype(bf16)
            rows = pl.ds(pl.multiple_of(c * QUARTER, 8), QUARTER)
            momentum_new[:, target] = outer_beta * mom_v[:, columns] + means[rows, :]


def exchange_kernel(
    grads,
    buffer,
    q_old,
    anchor,
    momentum,
    anchor_new,
    buffer_new,
    momentum_new,
    f_all,
    p_scaled,
    p_own,
    mom_all,
    grads_v,
    buffer_v,
    anchor_v,
    mom_v,
    means,
    nb,
    na,
    nk,
    q_v,
    mb,
    mp,
    qa,
    raw_b,
    gsend,
    g1,
    g2,
    g3,
    g4,
    gfull,
    rp,
    rown,
    r1,
    s1,
    r2,
    s2,
    s2b,
    r3,
    s3b,
    r4,
    p_all,
    load_sem,
    send_sem,
    recv_sem,
):
    c = lax.axis_index("island")
    h = lax.axis_index("fsdp_0")
    x = lax.axis_index("fsdp_1")
    y = lax.axis_index("fsdp_2")
    k = lax.axis_index("fsdp_3")
    z = h * 4 + c
    a = x * (1 - k) + y * k
    b = y * (1 - k) + x * k

    def first_axis(d):
        return {"fsdp_1": lax.rem(x + d * (1 - k), 4), "fsdp_2": lax.rem(y + d * k, 4)}

    def second_axis(d):
        return {"fsdp_1": lax.rem(x + d * k, 4), "fsdp_2": lax.rem(y + d * (1 - k), 4)}

    def along_z(d):
        to = lax.rem(z + d, 8)
        return {"fsdp_0": to // 4, "island": lax.rem(to, 4)}

    other_core = {"fsdp_3": 1 - k}
    other_half = {"fsdp_0": 1 - h}

    peers = [other_core, other_half]
    for d in (1, 2, 3):
        peers.append({"fsdp_1": lax.rem(x + d, 4)})
        peers.append({"fsdp_2": lax.rem(y + d, 4)})
        peers.append({"island": lax.rem(c + d, 4)})
    for d in (1, 2, 6, 7):
        peers.append(along_z(d))

    receives = iter(range(RECEIVES))
    free = list(range(SENDS))
    started = []

    def copy_to(src, dst, device, at=None, arrival=None):
        return pltpu.make_async_remote_copy(
            src_ref=src,
            dst_ref=dst,
            send_sem=send_sem.at[free.pop() if at is None else at],
            recv_sem=recv_sem.at[next(receives) if arrival is None else arrival],
            device_id=device,
            device_id_type=MESH,
        )

    def send(src, dst, device, arrival=None):
        at = free.pop()
        copy = copy_to(src, dst, device, at, arrival)
        copy.start()
        started.append((at, copy))
        return copy

    def sends_done():
        for at, copy in started:
            copy.wait_send()
            free.append(at)
        started.clear()

    barrier = pltpu.get_barrier_semaphore()
    for peer in peers:
        pl.semaphore_signal(barrier, inc=1, device_id=peer, device_id_type=MESH)

    loads = [
        pltpu.make_async_copy(momentum, mom_v, load_sem.at[0]),
        pltpu.make_async_copy(grads, grads_v, load_sem.at[1]),
        pltpu.make_async_copy(buffer, buffer_v, load_sem.at[2]),
        pltpu.make_async_copy(anchor, anchor_v, load_sem.at[3]),
        pltpu.make_async_copy(q_old, q_v, load_sem.at[4]),
    ]
    for at in (4, 0, 1, 2, 3):
        loads[at].start()
    loads[4].wait()
    qa[h, k, a, b] = q_v[...].astype(bf16)
    pl.semaphore_wait(barrier, len(peers))

    near_arrival, far_arrival = next(receives), next(receives)

    def along_second(part, arrival):
        for d in (2, 1, 3):
            send(part, part, second_axis(d), arrival)

    def first_sends(part):
        return {d: send(part, part, first_axis(d)) for d in (2, 1, 3)}

    own_piece = qa.at[h, k, a, b]
    far_piece = qa.at[1 - h, k, a, b]
    q_far = send(own_piece, own_piece, other_half)
    q_first = first_sends(own_piece)
    along_second(own_piece, near_arrival)

    line = []
    for step, first, rows in ((1, 0, 56), (2, 0, 40), (2, 40, 16), (3, 0, 24), (3, 24, 32)):
        up_ok = jnp.logical_and(c < 3, c >= step - 1)
        down_ok = jnp.logical_and(c > 0, c + step - 1 <= 3)
        up_part = mom_all.at[lax.rem(c - (step - 1) + 4, 4), pl.ds(first, rows)]
        down_part = mom_all.at[lax.rem(c + (step - 1), 4), pl.ds(first, rows)]
        up = copy_to(up_part, up_part, {"island": lax.rem(c + 1, 4)})
        down = copy_to(down_part, down_part, {"island": lax.rem(c + 3, 4)})
        line.append((up_ok, up, c - step >= 0, down_ok, down, c + step <= 3))

    def line_send(hop):
        up_ok, up, _, down_ok, down, _ = line[hop]

        @pl.when(up_ok)
        def _():
            up.start()

        @pl.when(down_ok)
        def _():
            down.start()

    def line_receive(hop):
        up_ok, up, from_below, down_ok, down, from_above = line[hop]

        @pl.when(from_below)
        def _():
            up.wait_recv()

        @pl.when(from_above)
        def _():
            down.wait_recv()

        @pl.when(up_ok)
        def _():
            up.wait_send()

        @pl.when(down_ok)
        def _():
            down.wait_send()

    loads[0].wait()
    mom_all[c] = mom_v[...].astype(bf16)
    line_send(0)

    loads[1].wait()
    loads[2].wait()

    low_lanes = lax.broadcasted_iota(jnp.int32, (16, 128), 1) < 64

    @pl.loop(0, OWN // 16)
    def _(i):
        at = pl.ds(pl.multiple_of(i * 16, 16), 16)
        matrix = grads_v[at, :].astype(f32) + buffer_v[at, :].astype(f32)
        mb[at, :] = matrix.astype(bf16)

        def block(half, row, column):
            first = (half * 16 + row * 4 + column) * 128
            return matrix[:, first : first + 128]

        for half in (0, 1):
            for outer in range(4):
                for pair in (0, 1):
                    lanes = slice((outer * 2 + pair) * 128, (outer * 2 + pair + 1) * 128)
                    one, two = block(half, outer, pair * 2), block(half, outer, pair * 2 + 1)
                    mp[half, 0, at, lanes] = jnp.where(
                        low_lanes, one, pltpu.roll(two, 64, 1)
                    ).astype(bf16)
                    one, two = block(half, pair * 2, outer), block(half, pair * 2 + 1, outer)
                    mp[half, 1, at, lanes] = jnp.where(
                        low_lanes, pltpu.roll(one, 64, 1), two
                    ).astype(bf16)

    mb[OWN:, :] = jnp.zeros((PADDED - OWN, COLS), bf16)
    for half in (0, 1):
        for core in (0, 1):
            mp[half, core, OWN:, :] = jnp.zeros((PADDED - OWN, COLS // 4), bf16)

    def arrived(at, copies, arrival):
        for d in (1, 3, 2):
            copies[d].wait_recv()
            along_second(qa.at[at, k, lax.rem(a + 4 - d, 4), b], arrival)

    arrived(h, q_first, near_arrival)
    q_far.wait_recv()
    q_first = first_sends(far_piece)
    along_second(far_piece, far_arrival)
    arrived(1 - h, q_first, far_arrival)
    q_cross = []
    for at, arrival in ((h, near_arrival), (1 - h, far_arrival)):
        twelve = qa.at[at, k, pl.ds(0, 3)]
        pltpu.make_async_remote_copy(
            src_ref=twelve,
            dst_ref=twelve,
            send_sem=send_sem.at[0],
            recv_sem=recv_sem.at[arrival],
            device_id=other_core,
            device_id_type=MESH,
        ).wait_recv()
        half = qa.at[at, k]
        q_cross.append((at, send(half, half, other_core)))

    line_receive(0)
    line_send(1)
    raw = jnp.zeros((PADDED, RANK), f32)
    for at, copy in q_cross:
        raw = raw + dot(mp[at, k], qa[at, k].reshape(COLS // 4, RANK), 1, 0)
        copy.wait_recv()
        raw = raw + dot(mp[at, 1 - k], qa[at, 1 - k].reshape(COLS // 4, RANK), 1, 0)
    raw_b[...] = raw.astype(bf16)
    raw_rows = raw_b[...]

    def total_of(parts):
        one, two, three, four = (parts[i].astype(f32) for i in range(4))
        return (one + two) + (three + four)

    sends_done()
    gram = dot(raw_rows, raw_rows, 0, 0)
    gsend[0] = gram[:64]
    gsend[1] = gram[64:]
    gram_cross = send(gsend.at[1 - k], g1, other_core)

    raw_t = raw.T.astype(bf16)

    def image(half, part, store):
        columns = pl.ds(pl.multiple_of(half * (COLS // 2) + part * 256, 256), 256)
        block = dot(raw_t, mb[:, columns], 1, 0)
        store(part * 2, block[:, :128])
        store(part * 2 + 1, block[:, 128:])

    def store_far(at, block):
        rp[at] = block.astype(bf16)

    def store_near(at, block):
        rown[at] = block

    r_cross = []
    for chunk in (0, 1):
        for part in range(chunk * 4, chunk * 4 + 4):
            image(1 - k, part, store_far)
        piece = pl.ds(chunk * 8, 8)
        r_cross.append(send(rp.at[piece], r1.at[piece], other_core))

    for part in range(8):
        image(k, part, store_near)

    gram_cross.wait_recv()
    g2[a] = (gsend[k] + g1[...]).astype(bf16)
    gram_first = [send(g2.at[a], g2.at[a], first_axis(d)) for d in (2, 1, 3)]

    for copy in r_cross:
        copy.wait_recv()
    r_first = []
    for d in (2, 1, 3):
        to = lax.rem(a + d, 4)
        for j in range(4):
            s1[d - 1, j] = (rown[to * 4 + j] + r1[to * 4 + j].astype(f32)).astype(bf16)
        r_first.append(send(s1.at[d - 1], r2.at[d - 1], first_axis(d)))

    for copy in gram_first:
        copy.wait_recv()
    g3[b] = total_of(g2).astype(bf16)
    gram_second = [send(g3.at[b], g3.at[b], second_axis(d)) for d in (2, 1, 3)]

    for copy in r_first:
        copy.wait_recv()
    for j in range(4):
        s2[j] = (rown[a * 4 + j] + r1[a * 4 + j].astype(f32)) + (
            (r2[0, j].astype(f32) + r2[1, j].astype(f32)) + r2[2, j].astype(f32)
        )
    r_second = []
    for d in (2, 1, 3):
        s2b[d - 1] = s2[lax.rem(b + d, 4)].astype(bf16)
        r_second.append(send(s2b.at[d - 1], r3.at[d - 1], second_axis(d)))

    for copy in gram_second:
        copy.wait_recv()
    g4[h] = total_of(g3).astype(bf16)
    gram_third = send(g4.at[h], g4.at[h], other_half)

    for copy in r_second:
        copy.wait_recv()
    s3b[...] = (
        s2[b] + ((r3[0].astype(f32) + r3[1].astype(f32)) + r3[2].astype(f32))
    ).astype(bf16)
    r_third = send(s3b, r4, other_half)
    line_receive(1)
    line_send(2)
    line_send(3)

    gram_third.wait_recv()
    gfull[k] = g4[0].astype(f32) + g4[1].astype(f32)
    gram_last = send(gfull.at[k], gfull.at[k], other_core)
    gram_last.wait_recv()
    lower = inverse_lower(jnp.concatenate([gfull[0], gfull[1]], axis=0))

    r_third.wait_recv()
    image_sum = s3b[...].astype(f32) + r4[...].astype(f32)
    factor = dot(lower, image_sum, 1, 0, precise).astype(bf16)
    f_all[k, a, b, 0] = factor
    squared = jnp.square(factor.astype(f32))
    nb[b, c] = dot(jnp.ones((8, RANK), f32), squared, 1, 1, precise)

    sends_done()
    square = nb.at[b, c]
    n_z = [send(square, square, along_z(d)) for d in (2, 1, 7)]
    z_copies = []
    for d, rows in ((2, pl.ds(0, 64)), (6, pl.ds(64, 64)), (1, pl.ds(0, 128)), (7, pl.ds(0, 128))):
        mine = f_all.at[k, a, b, 0, rows]
        z_copies.append(send(mine, f_all.at[k, a, b, (-d) % 4, rows], along_z(d)))

    up_a, down_a = first_axis(1), first_axis(3)
    up_b, down_b = second_axis(1), second_axis(3)
    a_below, a_above, a_far = lax.rem(a + 3, 4), lax.rem(a + 1, 4), lax.rem(a + 2, 4)
    b_below, b_above, b_far = lax.rem(b + 3, 4), lax.rem(b + 1, 4), lax.rem(b + 2, 4)

    def pass_on(at, islands, *devices):
        part = f_all.at[k, at[0], at[1], pl.ds(islands[0], islands[1] - islands[0])]
        return [send(part, part, device) for device in devices]

    early_b = pass_on((a, b), (0, 1), up_b, down_b)
    early_a = pass_on((a, b), (0, 1), up_a, down_a)
    basis = dot(raw_rows.astype(f32), lower, 1, 1, precise)[:OWN]
    p_all[c] = basis.astype(bf16)
    p_own[...] = (basis * (error_decay - 1.0)).astype(bf16)

    held = (f_all, p_scaled, p_own, mom_all, grads_v, buffer_v, anchor_v, mom_v)
    outs = (anchor_new, buffer_new, momentum_new)

    def finish(half, at):
        finish_columns(c, half, at, held, outs, means)

    for copy in early_b:
        copy.wait_recv()
    early_b_on = pass_on((a, b_above), (0, 1), down_b)
    early_below = pass_on((a, b_below), (0, 1), up_a, down_a)
    early_above = pass_on((a, b_above), (0, 1), up_a, down_a)
    for copy in early_a:
        copy.wait_recv()
    early_a_on = pass_on((a_above, b), (0, 1), down_a)

    for copy in n_z:
        copy.wait_recv()
    n_second = [send(nb.at[b], nb.at[b], second_axis(d)) for d in (2, 1, 3)]
    for copy in z_copies:
        copy.wait_recv()
    up_copy, down_copy = pass_on((a, b), (1, 4), up_b, down_b)
    p_copies = [send(p_all.at[c], p_all.at[c], {"island": lax.rem(c + d, 4)}) for d in (1, 2, 3)]
    for copy in n_second:
        copy.wait_recv()
    na[a] = (nb[0] + nb[1]) + (nb[2] + nb[3])
    n_first = [send(na.at[a], na.at[a], first_axis(d)) for d in (2, 1, 3)]
    own_up, own_down = pass_on((a, b), (1, 4), up_a, down_a)
    up_copy.wait_recv()
    b_on = pass_on((a, b_below), (2, 4), up_b)
    down_copy.wait_recv()
    b_on += pass_on((a, b_above), (1, 2), down_b)
    below_up, below_down = pass_on((a, b_below), (1, 4), up_a, down_a)
    above_up, above_down = pass_on((a, b_above), (1, 4), up_a, down_a)
    line_receive(2)
    line_send(4)
    for copy in early_b_on + b_on:
        copy.wait_recv()
    far_up, far_down = pass_on((a, b_far), (0, 4), up_a, down_a)
    own_up.wait_recv()
    own_on = pass_on((a_below, b), (2, 4), up_a)
    own_down.wait_recv()
    own_on += pass_on((a_above, b), (1, 2), down_a)
    for copy in n_first:
        copy.wait_recv()
    nk[k] = (na[0] + na[1]) + (na[2] + na[3])
    n_cross = send(nk.at[k], nk.at[k], other_core)

    def forward_a(at, early, up, down):
        for copy in early:
            copy.wait_recv()
        up.wait_recv()
        on = pass_on((a_below, at), (2, 4), up_a)
        down.wait_recv()
        return on + pass_on((a_above, at), (0, 2), down_a)

    def cross(at, arriving):
        for copy in arriving:
            copy.wait_recv()
        part = f_all.at[k, :, at]
        return send(part, part, other_core)

    below_on = forward_a(b_below, early_below, below_up, below_down)
    above_on = forward_a(b_above, early_above, above_up, above_down)
    far_on = forward_a(b_far, [], far_up, far_down)
    far_cross = []
    for i in (a, a_below, a_above, a_far):
        part = f_all.at[k, i, b_far]
        far_cross.append(copy_to(part, part, other_core))
    for copy in far_cross[:3]:
        copy.start()
    n_cross.wait_recv()
    for copy in p_copies:
        copy.wait_recv()
    rate = math.sqrt(ROWS * COLS / RANK) / 4.0
    for island in range(4):
        total = (nk[0, island] + nk[1, island])[:1]
        scale = rate * lax.rsqrt(total + epsilon)
        p_scaled[:, island * RANK : (island + 1) * RANK] = (
            p_all[island].astype(f32) * scale
        ).astype(bf16)
    loads[3].wait()
    crossing = [cross(b, early_a_on + own_on)]
    line_receive(3)
    line_receive(4)
    finish(k, b)
    crossing.append(cross(b_below, below_on))
    crossing.append(cross(b_above, above_on))
    finish(k, b_below)
    finish(k, b_above)
    crossing[0].wait_recv()
    finish(1 - k, a)
    for copy in far_on:
        copy.wait_recv()
    far_cross[3].start()
    crossing[1].wait_recv()
    finish(1 - k, a_below)
    finish(k, b_far)
    for copy in crossing[2:] + far_cross:
        copy.wait_recv()
    sends_done()
    for copy in far_cross:
        copy.wait_send()


def exchange(grads, buffer, q_old, anchor, momentum):
    vmem = pltpu.VMEM
    whole = pl.BlockSpec(memory_space=pltpu.VMEM)
    anywhere = pl.BlockSpec(memory_space=pltpu.HBM)
    block = (128, 128)
    return pl.pallas_call(
        exchange_kernel,
        out_shape=(
            vmem((OWN, COLS), bf16),
            vmem((OWN, COLS), bf16),
            vmem((QUARTER, COLS), f32),
            vmem((2, 4, 4, 4, *block), bf16),
            vmem((OWN, 4 * RANK), bf16),
            vmem((OWN, RANK), bf16),
            vmem((4, QUARTER, COLS), bf16),
            vmem((OWN, COLS), bf16),
            vmem((OWN, COLS), bf16),
            vmem((OWN, COLS), bf16),
            vmem((QUARTER, COLS), f32),
        ),
        in_specs=[anywhere] * 5,
        out_specs=(whole,) * 11,
        scratch_shapes=[
            vmem((OWN, 128), f32),
            vmem((4, 4, 8, 128), f32),
            vmem((4, 4, 8, 128), f32),
            vmem((2, 4, 8, 128), f32),
            vmem((64, RANK), f32),
            vmem((PADDED, COLS), bf16),
            vmem((2, 2, PADDED, COLS // 4), bf16),
            vmem((2, 2, 4, 4, 64, RANK), bf16),
            vmem((PADDED, RANK), bf16),
            vmem((2, 64, 128), f32),
            vmem((64, 128), f32),
            vmem((4, 64, 128), bf16),
            vmem((4, 64, 128), bf16),
            vmem((2, 64, 128), bf16),
            vmem((2, 64, 128), f32),
            vmem((16, *block), bf16),
            vmem((16, *block), f32),
            vmem((16, *block), bf16),
            vmem((3, 4, *block), bf16),
            vmem((3, 4, *block), bf16),
            vmem((4, *block), f32),
            vmem((3, *block), bf16),
            vmem((3, *block), bf16),
            vmem(block, bf16),
            vmem(block, bf16),
            vmem((4, OWN, RANK), bf16),
            pltpu.SemaphoreType.DMA((5,)),
            pltpu.SemaphoreType.DMA((SENDS,)),
            pltpu.SemaphoreType.DMA((RECEIVES,)),
        ],
        compiler_params=pltpu.CompilerParams(
            collective_id=0, has_side_effects=True, vmem_limit_bytes=32 * 1024 * 1024
        ),
        name="exchange",
    )(*(pltpu.with_memory_space_constraint(v, pltpu.HBM) for v in (grads, buffer, q_old, anchor, momentum)))


def update_kernel(*refs):
    done, held, outs, parts = refs[:3], refs[3:11], refs[11:14], refs[14:17]
    means, *sems = refs[17:]
    c = lax.axis_index("island")
    x = lax.axis_index("fsdp_1")
    y = lax.axis_index("fsdp_2")
    k = lax.axis_index("fsdp_3")
    a = x * (1 - k) + y * k

    def copy_columns(sources, first, to, width):
        for source, out, sem in zip(sources, outs, sems):
            copy = pltpu.make_async_copy(
                source.at[:, pl.ds(first, width)],
                out.at[:, pl.ds(to, width)],
                sem,
            )
            copy.start()

    for quarter in range(2):
        first = pl.multiple_of(k * (COLS // 2) + quarter * 1024, 1024)
        copy_columns(done, first, first, 1024)
    for at in (a, lax.rem(a + 3, 4)):
        for i in range(4):
            first = first_column(1 - k, i, at)
            copy_columns(done, first, first, 128)
    for n, at in enumerate((lax.rem(a + 1, 4), lax.rem(a + 2, 4))):
        finish_columns(c, 1 - k, at, held, parts, means, place=n * 4)
        for i in range(4):
            copy_columns(parts, (n * 4 + i) * 128, first_column(1 - k, i, at), 128)
    for source, out, sem in zip(done, outs, sems):
        pltpu.make_async_copy(source, out, sem).wait()


def update(*arrays):
    return pl.pallas_call(
        update_kernel,
        out_shape=(
            jax.ShapeDtypeStruct((OWN, COLS), bf16),
            jax.ShapeDtypeStruct((OWN, COLS), bf16),
            jax.ShapeDtypeStruct((QUARTER, COLS), f32),
        ),
        in_specs=[pl.BlockSpec(memory_space=pltpu.VMEM)] * 11,
        out_specs=[pl.BlockSpec(memory_space=pltpu.HBM)] * 3,
        scratch_shapes=[
            pltpu.VMEM((OWN, 1024), bf16),
            pltpu.VMEM((OWN, 1024), bf16),
            pltpu.VMEM((QUARTER, 1024), f32),
            pltpu.VMEM((OWN, 128), f32),
            pltpu.SemaphoreType.DMA,
            pltpu.SemaphoreType.DMA,
            pltpu.SemaphoreType.DMA,
        ],
        compiler_params=pltpu.CompilerParams(vmem_limit_bytes=8 * 1024 * 1024),
        name="update",
    )(*arrays)


def body(grads, buffer, q_old, anchor, momentum):
    anchor_new, buffer_new, momentum_new = update(
        *exchange(grads[0, 0], buffer[0], q_old[0], anchor, momentum)
    )
    return (anchor_new, buffer_new[None], momentum_new)


def solution(mesh):
    split = Mesh(
        mesh.devices.reshape(mesh.shape["island"], 2, 4, 4, 2),
        ("island", "fsdp_0", "fsdp_1", "fsdp_2", "fsdp_3"),
    )
    return jax.shard_map(
        body,
        mesh=split,
        in_specs=(
            P("island", None, FSDP, None),
            P("island", FSDP, None),
            P("island", FSDP, None),
            P(FSDP, None),
            P(FSDP_ISLAND, None),
        ),
        out_specs=(P(FSDP, None), P("island", FSDP, None), P(FSDP_ISLAND, None)),
        check_vma=False,
    )
```
